16 devices in a mesh: tp: 2 (over z), sp: 8 (over y, x, core).
Axes of the slice: x: 2, y: 2, z: 2, core: 2. Of those that a mesh axis runs over, the one named last changes fastest.
Arguments:
- x_tok: bfloat16 [256, 5120], replicated
- seq_lens: int32 [256], replicated
- k_cache: bfloat16 [256, 256, 8, 128], P(None, 'sp', 'tp')
- v_cache: bfloat16 [256, 256, 8, 128], P(None, 'sp', 'tp')
- g_attn: bfloat16 [5120], replicated
- w_q: bfloat16 [5120, 4096], P(None, 'tp')
- w_k: bfloat16 [5120, 1024], P(None, 'tp')
- w_v: bfloat16 [5120, 1024], P(None, 'tp')
- w_o: bfloat16 [4096, 5120], P('tp')
- g_mlp: bfloat16 [5120], replicated
- w_gate: bfloat16 [5120, 14336], P(None, 'tp')
- w_up: bfloat16 [5120, 14336], P(None, 'tp')
- w_down: bfloat16 [14336, 5120], P('tp')
Outputs:
- output 1: bfloat16 [256, 5120], replicated
- output 2: bfloat16 [256, 256, 8, 128], P(None, 'sp', 'tp')
- output 3: bfloat16 [256, 256, 8, 128], P(None, 'sp', 'tp')
All inputs are finite; a program needn't handle non-finite values.
Results may differ from the reference program's by a relative error of at most 0.013755.
Values sent between devices are 32-bit elements.
A program may use at most 1.25 GiB of HBM per device.

```python
import math
import jax
import jax.numpy as jnp
from jax import lax

MODEL_DIM = 5120
Q_HEADS = 32
KV_HEADS = 8
HEAD_DIM = 128
FF_DIM = 14336
BATCH_SIZE = 256
SEQ_LEN = 256

ROPE_BASE = 500000.0
NORM_EPS = 1e-5


def gauss_draw(rng_key, arr_shape):
    return jax.random.normal(rng_key, arr_shape, jnp.float32)


def draw_lens(rng_key):
    low_len = SEQ_LEN // 4
    key_len, key_hi, key_lo = jax.random.split(rng_key, 3)
    lens_raw = jax.random.randint(key_len, (BATCH_SIZE,), low_len, SEQ_LEN)
    idx_hi = jax.random.randint(key_hi, (), 0, BATCH_SIZE)
    idx_lo = (idx_hi + jax.random.randint(key_lo, (), 1, BATCH_SIZE)) % BATCH_SIZE
    row_ids = jnp.arange(BATCH_SIZE)
    lens_raw = jnp.where(row_ids == idx_hi, SEQ_LEN - 1, lens_raw)
    lens_raw = jnp.where(row_ids == idx_lo, low_len, lens_raw)
    return lens_raw.astype(jnp.int32)


def setup_inputs(seed: int = 0) -> dict:
    key_list = jax.random.split(jax.random.key(seed), 14)
    q_width = Q_HEADS * HEAD_DIM
    kv_width = KV_HEADS * HEAD_DIM
    groups = Q_HEADS // KV_HEADS
    cache_shape = (BATCH_SIZE, SEQ_LEN, KV_HEADS, HEAD_DIM)
    w_q32 = gauss_draw(key_list[4], (MODEL_DIM, q_width)) * MODEL_DIM ** -0.5
    self_gain = (math.log(SEQ_LEN) - 0.6) * math.sqrt(groups / HEAD_DIM)
    group_sum = jnp.sum(w_q32.reshape(MODEL_DIM, KV_HEADS, groups, HEAD_DIM), axis=2).reshape(MODEL_DIM, kv_width)
    w_k32 = group_sum * (self_gain / math.sqrt(groups)) + gauss_draw(key_list[5], (MODEL_DIM, kv_width)) * (0.5 * MODEL_DIM ** -0.5)
    value_scale = 0.5 * math.sqrt(SEQ_LEN)
    return {
        "x_tok": gauss_draw(key_list[0], (BATCH_SIZE, MODEL_DIM)).astype(jnp.bfloat16),
        "seq_lens": draw_lens(key_list[1]),
        "k_cache": gauss_draw(key_list[2], cache_shape).astype(jnp.bfloat16),
        "v_cache": (gauss_draw(key_list[3], cache_shape) * value_scale).astype(jnp.bfloat16),
        "g_attn": (1.0 + 0.2 * gauss_draw(key_list[6], (MODEL_DIM,))).astype(jnp.bfloat16),
        "w_q": w_q32.astype(jnp.bfloat16),
        "w_k": w_k32.astype(jnp.bfloat16),
        "w_v": (gauss_draw(key_list[7], (MODEL_DIM, kv_width)) * MODEL_DIM ** -0.5).astype(jnp.bfloat16),
        "w_o": (gauss_draw(key_list[8], (q_width, MODEL_DIM)) * q_width ** -0.5).astype(jnp.bfloat16),
        "g_mlp": (1.0 + 0.2 * gauss_draw(key_list[9], (MODEL_DIM,))).astype(jnp.bfloat16),
        "w_gate": (gauss_draw(key_list[10], (MODEL_DIM, FF_DIM)) * MODEL_DIM ** -0.5).astype(jnp.bfloat16),
        "w_up": (gauss_draw(key_list[11], (MODEL_DIM, FF_DIM)) * MODEL_DIM ** -0.5).astype(jnp.bfloat16),
        "w_down": (gauss_draw(key_list[12], (FF_DIM, MODEL_DIM)) * FF_DIM ** -0.5).astype(jnp.bfloat16),
    }


def rms_norm(x_in, norm_gain):
    x_f32 = x_in.astype(jnp.float32)
    inv_rms = lax.rsqrt(jnp.mean(x_f32 * x_f32, axis=-1, keepdims=True) + NORM_EPS)
    return (x_f32 * inv_rms * norm_gain.astype(jnp.float32)).astype(jnp.bfloat16)


def apply_rope(heads_in, positions):
    head_dim = heads_in.shape[-1]
    half_dim = head_dim // 2
    inv_freq = jnp.power(jnp.float32(ROPE_BASE), jnp.arange(half_dim, dtype=jnp.float32) * (-2.0 / head_dim))
    angles = positions.astype(jnp.float32)[:, None, None] * inv_freq
    cos_a = jnp.cos(angles)
    sin_a = jnp.sin(angles)
    heads_f32 = heads_in.astype(jnp.float32)
    first_half = heads_f32[..., :half_dim]
    second_half = heads_f32[..., half_dim:]
    rotated = jnp.concatenate([first_half * cos_a - second_half * sin_a, second_half * cos_a + first_half * sin_a], axis=-1)
    return rotated.astype(jnp.bfloat16)


def reference(x_tok, seq_lens, k_cache, v_cache, g_attn, w_q, w_k, w_v, w_o, g_mlp, w_gate, w_up, w_down):
    groups = Q_HEADS // KV_HEADS
    x_norm = rms_norm(x_tok, g_attn)
    q_new = jnp.dot(x_norm, w_q, preferred_element_type=jnp.float32).astype(jnp.bfloat16).reshape(BATCH_SIZE, Q_HEADS, HEAD_DIM)
    k_new = jnp.dot(x_norm, w_k, preferred_element_type=jnp.float32).astype(jnp.bfloat16).reshape(BATCH_SIZE, KV_HEADS, HEAD_DIM)
    v_new = jnp.dot(x_norm, w_v, preferred_element_type=jnp.float32).astype(jnp.bfloat16).reshape(BATCH_SIZE, KV_HEADS, HEAD_DIM)
    q_rot = apply_rope(q_new, seq_lens)
    k_rot = apply_rope(k_new, seq_lens)
    row_ids = jnp.arange(BATCH_SIZE)
    k_out = k_cache.at[row_ids, seq_lens].set(k_rot)
    v_out = v_cache.at[row_ids, seq_lens].set(v_new)
    score_scale = HEAD_DIM ** -0.5

    def attend_row(row_inputs):
        q_row, k_rows, v_rows, row_len = row_inputs
        scores = jnp.einsum("kgd,tkd->kgt", q_row.astype(jnp.float32), k_rows.astype(jnp.float32)) * score_scale
        is_valid = jnp.arange(SEQ_LEN) <= row_len
        masked = jnp.where(is_valid, scores, -jnp.inf)
        row_max = jnp.max(masked, axis=-1, keepdims=True)
        weights = jnp.exp(masked - row_max)
        row_sum = jnp.sum(weights, axis=-1, keepdims=True)
        mixed = jnp.einsum("kgt,tkd->kgd", weights.astype(jnp.bfloat16).astype(jnp.float32), v_rows.astype(jnp.float32))
        return (mixed / row_sum).astype(jnp.bfloat16)

    attn_heads = lax.map(attend_row, (q_rot.reshape(BATCH_SIZE, KV_HEADS, groups, HEAD_DIM), k_out, v_out, seq_lens))
    attn_flat = attn_heads.reshape(BATCH_SIZE, Q_HEADS * HEAD_DIM)
    attn_proj = jnp.dot(attn_flat, w_o, preferred_element_type=jnp.float32)
    hidden = (x_tok.astype(jnp.float32) + attn_proj).astype(jnp.bfloat16)
    h_norm = rms_norm(hidden, g_mlp)
    gate_proj = jnp.dot(h_norm, w_gate, preferred_element_type=jnp.float32).astype(jnp.bfloat16)
    up_proj = jnp.dot(h_norm, w_up, preferred_element_type=jnp.float32).astype(jnp.bfloat16)
    act_prod = (jax.nn.silu(gate_proj.astype(jnp.float32)) * up_proj.astype(jnp.float32)).astype(jnp.bfloat16)
    mlp_out = jnp.dot(act_prod, w_down, preferred_element_type=jnp.float32)
    y_out = (hidden.astype(jnp.float32) + mlp_out).astype(jnp.bfloat16)
    return (y_out, k_out, v_out)
```

```python
import functools

import jax
import jax.numpy as jnp
from jax import lax
from jax.experimental import pallas as pl
from jax.experimental.pallas import tpu as pltpu
from jax.sharding import PartitionSpec as P

ROPE_BASE = 500000.0
NORM_EPS = 1e-5
MESH = pl.DeviceIdType.MESH
VMEM_LIMIT = 60 * 1024 * 1024


def qkv_kernel(x_ref, g_ref, cos_ref, sin_ref, wq_ref, wk_ref, wv_ref, out_ref, u_ref, *, nq, nk):
    i = pl.program_id(0)

    @pl.when(i == 0)
    def _():
        xf = x_ref[...].astype(jnp.float32)
        inv = lax.rsqrt(jnp.mean(xf * xf, axis=-1, keepdims=True) + NORM_EPS)
        u_ref[...] = (xf * inv * g_ref[...].astype(jnp.float32)).astype(jnp.bfloat16)

    def project(w_ref, rope):
        y = jnp.dot(u_ref[...], w_ref[...], preferred_element_type=jnp.float32)
        y = y.astype(jnp.bfloat16)
        if rope:
            for h in range(y.shape[1] // 128):
                t = y[:, h * 128 : (h + 1) * 128].astype(jnp.float32)
                r = t * cos_ref[...] + pltpu.roll(t, 64, 1) * sin_ref[...]
                out_ref[:, h * 128 : (h + 1) * 128] = r.astype(jnp.bfloat16)
        else:
            out_ref[...] = y

    @pl.when(i < nq)
    def _():
        project(wq_ref, True)

    @pl.when(jnp.logical_and(i >= nq, i < nq + nk))
    def _():
        project(wk_ref, True)

    @pl.when(i >= nq + nk)
    def _():
        project(wv_ref, False)


def qkv_call(x_tok, g_attn, cos_f, sin_f, wq, wk, wv):
    rows, dim = x_tok.shape
    bn = 256
    nq, nk, nv = wq.shape[1] // bn, wk.shape[1] // bn, wv.shape[1] // bn
    whole = lambda i: (0, 0)
    return pl.pallas_call(
        functools.partial(qkv_kernel, nq=nq, nk=nk),
        grid=(nq + nk + nv,),
        in_specs=[
            pl.BlockSpec((rows, dim), whole),
            pl.BlockSpec((1, dim), whole),
            pl.BlockSpec((rows, 128), whole),
            pl.BlockSpec((rows, 128), whole),
            pl.BlockSpec((dim, bn), lambda i: (0, jnp.minimum(i, nq - 1))),
            pl.BlockSpec((dim, bn), lambda i: (0, jnp.clip(i - nq, 0, nk - 1))),
            pl.BlockSpec((dim, bn), lambda i: (0, jnp.clip(i - nq - nk, 0, nv - 1))),
        ],
        out_specs=pl.BlockSpec((rows, bn), lambda i: (0, i)),
        out_shape=jax.ShapeDtypeStruct((rows, (nq + nk + nv) * bn), jnp.bfloat16),
        scratch_shapes=[pltpu.VMEM((rows, dim), jnp.bfloat16)],
        compiler_params=pltpu.CompilerParams(vmem_limit_bytes=VMEM_LIMIT),
        name="qkv",
    )(x_tok, g_attn.reshape(1, dim), cos_f, sin_f, wq, wk, wv)


PAIRS = 8


def att_kernel(lens_ref, base_ref, q_ref, kn_ref, vn_ref, k_ref, v_ref, ko_ref, vo_ref, mix_ref, m_ref, l_ref):
    step = pl.program_id(0)
    base = base_ref[0]

    @pl.when(step == 0)
    def _():
        m_ref[...] = jnp.zeros_like(m_ref)
        l_ref[...] = jnp.zeros_like(l_ref)

    row = lax.broadcasted_iota(jnp.int32, (128, 128), 0)
    row_pos = base + row // 4
    ri = lax.broadcasted_iota(jnp.int32, (32, 256), 0)
    ci = lax.broadcasted_iota(jnp.int32, (32, 256), 1)
    same = jnp.logical_and(ri // 16 == ci // 128, (ri % 16) // 4 == ci % 4)
    col_pos = jnp.where(same, base + (ci % 128) // 4, 1 << 30)
    first = ri < 16
    lane = lax.broadcasted_iota(jnp.int32, (32, 128), 1)
    scale = 128.0 ** -0.5
    m_all, l_all = m_ref[...], l_ref[...]
    for j in range(PAIRS):
        pair = step * PAIRS + j
        p0 = lens_ref[2 * pair]
        p1 = lens_ref[2 * pair + 1]
        ks, vs = [], []
        for t, p in ((0, p0), (1, p1)):
            b = 2 * j + t
            hit = row_pos == p
            for src, new, dst, acc in ((k_ref, kn_ref, ko_ref, ks), (v_ref, vn_ref, vo_ref, vs)):
                old = src[b].astype(jnp.float32)
                add = jnp.broadcast_to(new[b][None], (16, 8, 128)).reshape(128, 128)
                val = jnp.where(hit, add, old).astype(jnp.bfloat16)
                dst[b] = val
                acc.append(val)
        kk = jnp.concatenate(ks, axis=0)
        vv = jnp.concatenate(vs, axis=0)
        s = lax.dot_general(q_ref[j], kk, (((1,), (1,)), ((), ())), preferred_element_type=jnp.float32) * scale
        valid = col_pos <= jnp.where(first, p0, p1)
        s = jnp.where(valid, s, -1e30)
        m = jnp.max(s, axis=1, keepdims=True)
        w = jnp.where(valid, jnp.exp(s - m), 0.0)
        l = jnp.sum(w, axis=1, keepdims=True)
        mix_ref[j] = jnp.dot(w.astype(jnp.bfloat16), vv, preferred_element_type=jnp.float32)
        m_all = jnp.where(lane == pair, m, m_all)
        l_all = jnp.where(lane == pair, l, l_all)
    m_ref[...] = m_all
    l_ref[...] = l_all


def att_call(seq_lens, base, q, kn, vn, k2, v2):
    batch = k2.shape[0]
    nb = 2 * PAIRS
    blk = lambda i, *_: (i, 0, 0)
    grid_spec = pltpu.PrefetchScalarGridSpec(
        num_scalar_prefetch=2,
        grid=(batch // nb,),
        in_specs=[
            pl.BlockSpec((PAIRS, 32, 128), blk),
            pl.BlockSpec((nb, 8, 128), blk),
            pl.BlockSpec((nb, 8, 128), blk),
            pl.BlockSpec((nb, 128, 128), blk),
            pl.BlockSpec((nb, 128, 128), blk),
        ],
        out_specs=[
            pl.BlockSpec((nb, 128, 128), blk),
            pl.BlockSpec((nb, 128, 128), blk),
            pl.BlockSpec((PAIRS, 32, 128), blk),
            pl.BlockSpec((32, 128), lambda i, *_: (0, 0)),
            pl.BlockSpec((32, 128), lambda i, *_: (0, 0)),
        ],
    )
    return pl.pallas_call(
        att_kernel,
        grid_spec=grid_spec,
        out_shape=[
            jax.ShapeDtypeStruct(k2.shape, jnp.bfloat16),
            jax.ShapeDtypeStruct(v2.shape, jnp.bfloat16),
            jax.ShapeDtypeStruct((batch // 2, 32, 128), jnp.float32),
            jax.ShapeDtypeStruct((32, 128), jnp.float32),
            jax.ShapeDtypeStruct((32, 128), jnp.float32),
        ],
        compiler_params=pltpu.CompilerParams(vmem_limit_bytes=VMEM_LIMIT),
        name="att",
    )(seq_lens, base, q, kn, vn, k2, v2)


def coords():
    z = lax.axis_index("tp")
    sp = lax.axis_index("sp")
    return z, sp // 4, (sp // 2) % 2, sp % 2


def device(z, y, x, c):
    return (z, y * 4 + x * 2 + c)


def flip(a, on):
    return 1 - a if on else a


def greet(peers):
    barrier = pltpu.get_barrier_semaphore()
    for p in peers:
        pl.semaphore_signal(barrier, inc=1, device_id=p, device_id_type=MESH)
    pl.semaphore_wait(barrier, len(peers))


def remote(src, dst, send, recv, dev):
    return pltpu.make_async_remote_copy(src_ref=src, dst_ref=dst, send_sem=send, recv_sem=recv, device_id=dev, device_id_type=MESH)


def combine_kernel(mix_ref, m_ref, l_ref, o_ref, got1, st_own, st1, comb, stc, got2, st2, s1, r1, s2, r2):
    z, y, x, c = coords()
    partner = device(z, y, x, 1 - c)
    chips = [(y, x), (y, 1 - x), (1 - y, x), (1 - y, 1 - x)]
    greet([partner] + [device(z, b, a, c) for b, a in chips[1:]])

    st_own[0] = m_ref[...]
    st_own[1] = l_ref[...]
    first = []
    for k in (1, 2, 3, 0):
        b, a = chips[k]
        start = 16 * (b * 4 + a * 2 + 1 - c)
        first.append(remote(mix_ref.at[pl.ds(start, 16)], got1.at[k], s1.at[k], r1.at[k], partner))
    stat1 = remote(st_own, st1, s1.at[4], r1.at[4], partner)
    stat1.start()
    for cp in first:
        cp.start()
    stat1.wait_recv()
    ma, mb = st_own[0], st1[0]
    mg = jnp.maximum(ma, mb)
    fa, fb = jnp.exp(ma - mg), jnp.exp(mb - mg)
    stc[0] = mg
    stc[1] = st_own[1] * fa + st1[1] * fb
    second = {}
    stats2 = {}
    for k in (1, 2, 3):
        b, a = chips[k]
        stats2[k] = remote(stc, st2.at[k - 1], s2.at[3 + k - 1], r2.at[3 + k - 1], device(z, b, a, c))
        stats2[k].start()
    for n, k in enumerate((1, 2, 3, 0)):
        b, a = chips[k]
        block = b * 4 + a * 2 + c
        back = (128 - 16 * block) % 128
        ga, gb = pltpu.roll(fa, back, 1), pltpu.roll(fb, back, 1)
        first[n].wait_recv()
        for j in range(16):
            comb[k, j] = mix_ref[16 * block + j] * ga[:, j : j + 1] + got1[k, j] * gb[:, j : j + 1]
        if k:
            second[k] = remote(comb.at[k], got2.at[k - 1], s2.at[k - 1], r2.at[k - 1], device(z, b, a, c))
            second[k].start()
    for k in (1, 2, 3):
        stats2[k].wait_recv()
    ms = [stc[0]] + [st2[k, 0] for k in range(3)]
    ls = [stc[1]] + [st2[k, 1] for k in range(3)]
    mg = jnp.maximum(jnp.maximum(ms[0], ms[1]), jnp.maximum(ms[2], ms[3]))
    fs = [jnp.exp(m - mg) for m in ms]
    total = ls[0] * fs[0] + ls[1] * fs[1] + ls[2] * fs[2] + ls[3] * fs[3]
    block = y * 4 + x * 2 + c
    back = (128 - 16 * block) % 128
    fs = [pltpu.roll(f, back, 1) for f in fs]
    total = pltpu.roll(total, back, 1)
    for k in (1, 2, 3):
        second[k].wait_recv()
    for j in range(16):
        acc = comb[0, j] * fs[0][:, j : j + 1]
        for k in (1, 2, 3):
            acc = acc + got2[k - 1, j] * fs[k][:, j : j + 1]
        o_ref[j] = (acc / total[:, j : j + 1]).astype(jnp.bfloat16)
    for cp in first + [stat1] + [stats2[k] for k in stats2] + [second[k] for k in second]:
        cp.wait_send()


def combine_call(mix, m, l):
    vm = pl.BlockSpec(memory_space=pltpu.VMEM)
    f32 = jnp.float32
    return pl.pallas_call(
        combine_kernel,
        out_shape=jax.ShapeDtypeStruct((16, 32, 128), jnp.bfloat16),
        in_specs=[vm, vm, vm],
        out_specs=vm,
        scratch_shapes=[
            pltpu.VMEM((4, 16, 32, 128), f32),
            pltpu.VMEM((2, 32, 128), f32),
            pltpu.VMEM((2, 32, 128), f32),
            pltpu.VMEM((4, 16, 32, 128), f32),
            pltpu.VMEM((2, 32, 128), f32),
            pltpu.VMEM((3, 16, 32, 128), f32),
            pltpu.VMEM((3, 2, 32, 128), f32),
            pltpu.SemaphoreType.DMA((5,)),
            pltpu.SemaphoreType.DMA((5,)),
            pltpu.SemaphoreType.DMA((6,)),
            pltpu.SemaphoreType.DMA((6,)),
        ],
        compiler_params=pltpu.CompilerParams(collective_id=0, has_side_effects=True, vmem_limit_bytes=VMEM_LIMIT),
        name="combine",
    )(mix, m, l)


def hidden_kernel(part_ref, x_ref, g_ref, h_ref, hid_ref, zb, hbuf, sz, rz, ss, rs, sd, rd):
    z, y, x, c = coords()
    partner = device(z, y, x, 1 - c)
    zdev = device(1 - z, y, x, c)
    z1, x1 = z + c * (1 - 2 * z), x + (1 - c) * (1 - 2 * x)
    z2, x2 = z + (1 - c) * (1 - 2 * z), x + c * (1 - 2 * x)
    dev1, dev2 = device(z1, y, x1, c), device(z2, y, x2, c)
    greet([partner, dev1, dev2])
    cz = remote(part_ref.at[pl.ds(16 * (1 - z), 16)], zb, sz, rz, zdev)
    cz.start()
    cz.wait_recv()
    own = part_ref[pl.ds(pl.multiple_of(16 * z, 16), 16), :]
    hid = (x_ref[...].astype(jnp.float32) + (own + zb[...])).astype(jnp.bfloat16).astype(jnp.float32)
    hid_ref[...] = hid
    inv = lax.rsqrt(jnp.mean(hid * hid, axis=-1, keepdims=True) + NORM_EPS)
    slot = lambda zz, xx, cc: (xx * 2 + cc) * 2 + zz
    mine = slot(z, x, c)
    hbuf[mine] = (hid * inv * g_ref[...].astype(jnp.float32)).astype(jnp.bfloat16).astype(jnp.float32)

    def send(sl, dev, s, r, n):
        cp = remote(hbuf.at[sl], hbuf.at[sl], s.at[n], r.at[n], dev)
        cp.start()
        return cp

    a1 = send(mine, dev1, ss, rs, 0)
    a2 = send(mine, dev2, ss, rs, 1)
    d0 = send(mine, partner, sd, rd, 0)
    a1.wait_recv()
    s1 = slot(z1, x1, c)
    a3 = send(s1, dev2, ss, rs, 2)
    d1 = send(s1, partner, sd, rd, 1)
    a2.wait_recv()
    d2 = send(slot(z2, x2, c), partner, sd, rd, 2)
    a3.wait_recv()
    d3 = send(slot(1 - z, 1 - x, c), partner, sd, rd, 3)
    for cp in (d0, d1, d2, d3):
        cp.wait_recv()
    for k in range(8):
        h_ref[pl.ds(16 * k, 16), :] = hbuf[k].astype(jnp.bfloat16)
    for cp in (cz, a1, a2, a3, d0, d1, d2, d3):
        cp.wait_send()


def hidden_call(part, xs, g):
    vm = pl.BlockSpec(memory_space=pltpu.VMEM)
    f32 = jnp.float32
    dim = part.shape[1]
    dma = pltpu.SemaphoreType.DMA
    return pl.pallas_call(
        hidden_kernel,
        out_shape=[jax.ShapeDtypeStruct((128, dim), jnp.bfloat16), jax.ShapeDtypeStruct((16, dim), f32)],
        in_specs=[vm, vm, vm],
        out_specs=[vm, vm],
        scratch_shapes=[
            pltpu.VMEM((16, dim), f32),
            pltpu.VMEM((8, 16, dim), f32),
            dma, dma, dma((3,)), dma((3,)), dma((4,)), dma((4,)),
        ],
        compiler_params=pltpu.CompilerParams(collective_id=1, has_side_effects=True, vmem_limit_bytes=VMEM_LIMIT),
        name="hidden",
    )(part, xs, g.reshape(1, dim))


def gate_up_kernel(idx_ref, h_ref, wg_ref, wu_ref, m_ref):
    g = jnp.dot(h_ref[...], wg_ref[...], preferred_element_type=jnp.float32).astype(jnp.bfloat16).astype(jnp.float32)
    u = jnp.dot(h_ref[...], wu_ref[...], preferred_element_type=jnp.float32).astype(jnp.bfloat16).astype(jnp.float32)
    m_ref[...] = (jax.nn.silu(g) * u).astype(jnp.bfloat16)


def gate_up_call(idx, h, wg, wu, ways):
    rows, dim = h.shape
    bn = 256
    steps = wg.shape[1] // ways // bn
    wspec = pl.BlockSpec((dim, bn), lambda i, s: (0, s[0] * steps + i))
    return pl.pallas_call(
        gate_up_kernel,
        grid_spec=pltpu.PrefetchScalarGridSpec(
            num_scalar_prefetch=1,
            grid=(steps,),
            in_specs=[pl.BlockSpec((rows, dim), lambda i, s: (0, 0)), wspec, wspec],
            out_specs=pl.BlockSpec((rows, bn), lambda i, s: (0, i)),
        ),
        out_shape=jax.ShapeDtypeStruct((rows, steps * bn), jnp.bfloat16),
        compiler_params=pltpu.CompilerParams(vmem_limit_bytes=VMEM_LIMIT),
        name="gate_up",
    )(idx, h, wg, wu)


def down_kernel(idx_ref, m_ref, wd_ref, o_ref):
    o_ref[...] = jnp.dot(m_ref[...], wd_ref[...], preferred_element_type=jnp.float32)


def down_call(idx, m, wd):
    rows, depth = m.shape
    bn = 512
    return pl.pallas_call(
        down_kernel,
        grid_spec=pltpu.PrefetchScalarGridSpec(
            num_scalar_prefetch=1,
            grid=(wd.shape[1] // bn,),
            in_specs=[pl.BlockSpec((rows, depth), lambda i, s: (0, 0)), pl.BlockSpec((depth, bn), lambda i, s: (s[0], i))],
            out_specs=pl.BlockSpec((rows, bn), lambda i, s: (0, i)),
        ),
        out_shape=jax.ShapeDtypeStruct((rows, wd.shape[1]), jnp.float32),
        compiler_params=pltpu.CompilerParams(vmem_limit_bytes=VMEM_LIMIT),
        name="down",
    )(idx, m, wd)


COLORS = ((0, 1664), (1664, 1664), (3328, 1792))


def output_kernel(part_ref, hid_ref, y_ref, got1, acc, got2, ybuf, s1, r1, s2, r2, sl, rl, sd, rd):
    z, y, x, c = coords()
    partner = device(z, y, x, 1 - c)
    chips = [(z, x), (z, 1 - x), (1 - z, x), (1 - z, 1 - x)]
    near = [device(z, y, 1 - x, c), device(z, 1 - y, x, c), device(1 - z, y, x, c)]
    greet([partner] + near + [device(1 - z, y, 1 - x, c)])
    slot = lambda zz, xx, cc: (xx * 2 + cc) * 2 + zz
    rows16 = lambda s: pl.ds(pl.multiple_of(16 * s, 16), 16)
    order = (3, 1, 2, 0)
    first = {}
    for k in order:
        zz, xx = chips[k]
        first[k] = remote(part_ref.at[rows16(slot(zz, xx, 1 - c))], got1.at[k], s1.at[k], r1.at[k], partner)
        first[k].start()
    second = {}
    for k in order:
        zz, xx = chips[k]
        first[k].wait_recv()
        acc[k] = part_ref[rows16(slot(zz, xx, c)), :] + got1[k]
        if k:
            second[k] = remote(acc.at[k], got2.at[k - 1], s2.at[k - 1], r2.at[k - 1], device(zz, y, xx, c))
            second[k].start()
    for k in (1, 2, 3):
        second[k].wait_recv()
    total = (acc[0] + got2[0]) + (got2[1] + got2[2])
    mine = y * 8 + slot(z, x, c)
    ybuf[mine] = (hid_ref[...] + total).astype(jnp.bfloat16).astype(jnp.float32)

    def shard(mask):
        zz, yy, xx = flip(z, mask & 4), flip(y, mask & 2), flip(x, mask & 1)
        return yy * 8 + slot(zz, xx, c)

    links, locals_ = {}, {}

    def piece(mask, k):
        return ybuf.at[shard(mask), :, pl.ds(*COLORS[k])]

    def push(mask, k, dim):
        n = 7 * k + (mask | (1 << dim)) - 1
        cp = remote(piece(mask, k), piece(mask, k), sl.at[n], rl.at[n], near[dim])
        cp.start()
        links[k, mask | (1 << dim)] = cp

    def across(mask, k):
        n = 8 * k + mask
        cp = remote(piece(mask, k), piece(mask, k), sd.at[n], rd.at[n], partner)
        cp.start()
        locals_[k, mask] = cp

    turn = lambda k: [(k + i) % 3 for i in range(3)]
    for i in range(3):
        for k in range(3):
            push(0, k, turn(k)[i])
    for k in range(3):
        across(0, k)
    for level in ((0,), (1,), (0, 1), (2,), (0, 2), (1, 2), (0, 1, 2)):
        for k in range(3):
            dims = turn(k)
            mask = sum(1 << dims[i] for i in level)
            links[k, mask].wait_recv()
            for i in range(max(level) + 1, 3):
                push(mask, k, dims[i])
            across(mask, k)
    for cp in locals_.values():
        cp.wait_recv()
    for s in range(16):
        y_ref[pl.ds(16 * s, 16), :] = ybuf[s].astype(jnp.bfloat16)
    for cp in list(first.values()) + list(second.values()) + list(links.values()) + list(locals_.values()):
        cp.wait_send()


def output_call(part, hid):
    vm = pl.BlockSpec(memory_space=pltpu.VMEM)
    f32 = jnp.float32
    dim = part.shape[1]
    dma = pltpu.SemaphoreType.DMA
    return pl.pallas_call(
        output_kernel,
        out_shape=jax.ShapeDtypeStruct((256, dim), jnp.bfloat16),
        in_specs=[vm, vm],
        out_specs=vm,
        scratch_shapes=[
            pltpu.VMEM((4, 16, dim), f32),
            pltpu.VMEM((4, 16, dim), f32),
            pltpu.VMEM((3, 16, dim), f32),
            pltpu.VMEM((16, 16, dim), f32),
            dma((4,)), dma((4,)), dma((3,)), dma((3,)), dma((21,)), dma((21,)), dma((24,)), dma((24,)),
        ],
        compiler_params=pltpu.CompilerParams(collective_id=2, has_side_effects=True, vmem_limit_bytes=VMEM_LIMIT),
        name="output",
    )(part, hid)


def solution(mesh):
    cache_spec = P(None, "sp", "tp", None)
    col_spec = P(None, "tp")
    row_spec = P("tp", None)
    full_spec = P()

    def local_step(x_tok, seq_lens, k_blk, v_blk, g_attn, wq_loc, wk_loc, wv_loc, wo_loc, g_mlp, wg_loc, wu_loc, wd_loc):
        batch, seq_blk, kv_loc, head_dim = k_blk.shape
        q_loc = wq_loc.shape[1] // head_dim
        half = head_dim // 2
        z, sp = lax.axis_index("tp"), lax.axis_index("sp")
        inv_freq = jnp.power(jnp.float32(ROPE_BASE), jnp.arange(half, dtype=jnp.float32) * (-2.0 / head_dim))
        angles = seq_lens.astype(jnp.float32)[:, None] * inv_freq
        cos_a, sin_a = jnp.cos(angles), jnp.sin(angles)
        cos_f = jnp.concatenate([cos_a, cos_a], axis=-1)
        sin_f = jnp.concatenate([-sin_a, sin_a], axis=-1)
        qkv = qkv_call(x_tok, g_attn, cos_f, sin_f, wq_loc, wk_loc, wv_loc)
        qw, kw = q_loc * head_dim, kv_loc * head_dim
        q = qkv[:, :qw].reshape(batch // 2, 2 * q_loc, head_dim)
        twice = lambda t: jnp.concatenate([t, t], axis=1).astype(jnp.float32)
        kn = twice(qkv[:, qw : qw + kw].reshape(batch, kv_loc, head_dim))
        vn = twice(qkv[:, qw + kw :].reshape(batch, kv_loc, head_dim))
        base = (sp * seq_blk).astype(jnp.int32).reshape(1)
        flat = (batch, seq_blk * kv_loc, head_dim)
        k_out, v_out, mix, m, l = att_call(seq_lens, base, q, kn, vn, k_blk.reshape(flat), v_blk.reshape(flat))
        o = combine_call(mix, m, l).reshape(32, q_loc * head_dim)
        part = jnp.dot(o, wo_loc, preferred_element_type=jnp.float32)
        xs = lax.dynamic_slice_in_dim(x_tok, 32 * sp + 16 * z, 16, 0)
        h, hid = hidden_call(part, xs, g_mlp)
        idx = (sp % 4).astype(jnp.int32).reshape(1)
        act = gate_up_call(idx, h, wg_loc, wu_loc, 4)
        down = down_call(idx, act, wd_loc)
        y_out = output_call(down, hid)
        return y_out, k_out.reshape(k_blk.shape), v_out.reshape(v_blk.shape)

    return jax.shard_map(local_step, mesh=mesh, in_specs=(full_spec, full_spec, cache_spec, cache_spec, full_spec, col_spec, col_spec, col_spec, row_spec, full_spec, col_spec, col_spec, row_spec), out_specs=(full_spec, cache_spec, cache_spec), check_vma=False)
```

```python
import jax
import jax.numpy as jnp
import numpy as np
from jax import lax
from jax.experimental import pallas as pl
from jax.experimental.pallas import tpu as pltpu
from jax.sharding import PartitionSpec as P

ROPE_BASE = 500000.0
NORM_EPS = 1e-5
MESH = pl.DeviceIdType.MESH
VMEM_LIMIT = 60 * 1024 * 1024


WN = 256
RB = 32
RING = 4
PAIRS = 8


def attend_kernel(lens_s, lens_ref, freq_ref, g_ref, x_hbm, wq, wk, wv, kc, vc, ko, vo, mix_ref, m_ref, l_ref,
                  xb, u, wbuf, q_s, kn_s, vn_s, cos_s, sin_s, kbuf, vbuf, sx, sw, sk, sv, tk, tv):
    rows, dim = xb.shape
    nq, nk, nv = wq.shape[1] // WN, wk.shape[1] // WN, wv.shape[1] // WN
    blocks = kc.shape[0] // RB
    base = lax.axis_index("sp") * (kc.shape[1] // 4)

    cx = pltpu.make_async_copy(x_hbm, xb, sx)
    cx.start()

    def weight(w, i, n):
        return pltpu.make_async_copy(w.at[:, pl.ds(pl.multiple_of(i * WN, WN), WN)], wbuf.at[n], sw.at[n])

    for i in range(nq):
        weight(wq, i, i).start()
    for i in range(nk):
        weight(wk, i, nq + i).start()
    for i in range(nv):
        weight(wv, i, nq + nk + i).start()

    def load(n):
        r, t = pl.ds(n * RB, RB), n % RING
        return pltpu.make_async_copy(kc.at[r], kbuf.at[t], sk.at[t]), pltpu.make_async_copy(vc.at[r], vbuf.at[t], sv.at[t])

    def store(n):
        r, t = pl.ds(n * RB, RB), n % RING
        return pltpu.make_async_copy(kbuf.at[t], ko.at[r], tk.at[t]), pltpu.make_async_copy(vbuf.at[t], vo.at[r], tv.at[t])

    for n in range(RING):
        for cp in load(n):
            cp.start()

    eye = lax.broadcasted_iota(jnp.int32, (rows, rows), 0) == lax.broadcasted_iota(jnp.int32, (rows, rows), 1)
    lens_f = lens_ref[...].astype(jnp.float32).reshape(1, rows)
    pos = jnp.sum(jnp.where(eye, lens_f, 0.0), axis=1, keepdims=True)
    angles = pos * freq_ref[...]
    half = lax.broadcasted_iota(jnp.int32, (rows, 128), 1) < 64
    cos_s[...] = jnp.cos(angles)
    sin_a = jnp.sin(angles)
    sin_s[...] = jnp.where(half, -sin_a, sin_a)
    m_ref[...] = jnp.zeros_like(m_ref)
    l_ref[...] = jnp.zeros_like(l_ref)

    cx.wait()
    gain = g_ref[...].astype(jnp.float32).reshape(1, dim)

    def norm(i, carry):
        r = pl.ds(pl.multiple_of(i * 32, 32), 32)
        xf = xb[r, :].astype(jnp.float32)
        inv = lax.rsqrt(jnp.mean(xf * xf, axis=-1, keepdims=True) + NORM_EPS)
        u[r, :] = (xf * inv * gain).astype(jnp.bfloat16)
        return carry

    lax.fori_loop(0, rows // 32, norm, 0)

    def rope(t):
        return (t * cos_s[...] + pltpu.roll(t, 64, 1) * sin_s[...]).astype(jnp.bfloat16).astype(jnp.float32)

    def project(w, i, n):
        weight(w, i, n).wait()
        y = jnp.dot(u[...], wbuf[n], preferred_element_type=jnp.float32)
        return y.astype(jnp.bfloat16).astype(jnp.float32)

    def q_chunk(i, carry):
        y = project(wq, i, i)
        for t in range(WN // 128):
            q_s[pl.ds(i * (WN // 128) + t, rows, stride=16), :] = rope(y[:, t * 128 : (t + 1) * 128])
        return carry

    lax.fori_loop(0, nq, q_chunk, 0)
    for w, count, first, dst, turn in ((wk, nk, nq, kn_s, True), (wv, nv, nq + nk, vn_s, False)):

        def kv_chunk(i, carry, w=w, first=first, dst=dst, turn=turn):
            y = project(w, i, first + i)
            for t in range(WN // 128):
                head = y[:, t * 128 : (t + 1) * 128]
                head = rope(head) if turn else head
                for again in (0, 4):
                    dst[pl.ds(i * (WN // 128) + t + again, rows, stride=8), :] = head
            return carry

        lax.fori_loop(0, count, kv_chunk, 0)

    row_pos = base + lax.broadcasted_iota(jnp.int32, (128, 128), 0) // 4
    ri = lax.broadcasted_iota(jnp.int32, (32, 256), 0)
    ci = lax.broadcasted_iota(jnp.int32, (32, 256), 1)
    same = jnp.logical_and(ri // 16 == ci // 128, (ri % 16) // 4 == ci % 4)
    col_pos = jnp.where(same, base + (ci % 128) // 4, 1 << 30)
    upper = ri < 16
    lane = lax.broadcasted_iota(jnp.int32, (32, 128), 1)
    scale = 128.0 ** -0.5

    for n in range(blocks):
        slot = n % RING
        for cp in load(n):
            cp.wait()

        def group(g, carry, n=n, slot=slot):
            m_all, l_all = m_ref[...], l_ref[...]
            for j in range(PAIRS):
                local = g * PAIRS + j
                pair = n * (RB // 2) + local
                p0 = lens_s[2 * pair]
                p1 = lens_s[2 * pair + 1]
                ks, vs = [], []
                for t, p in ((0, p0), (1, p1)):
                    b = 2 * local + t
                    new = pl.ds(pl.multiple_of(8 * (2 * pair + t), 8), 8)
                    hit = row_pos == p
                    for buf, fresh, acc in ((kbuf, kn_s, ks), (vbuf, vn_s, vs)):
                        old = buf[slot, b].astype(jnp.float32)
                        add = jnp.broadcast_to(fresh[new, :][None], (16, 8, 128)).reshape(128, 128)
                        val = jnp.where(hit, add, old).astype(jnp.bfloat16)
                        buf[slot, b] = val
                        acc.append(val)
                kk = jnp.concatenate(ks, axis=0)
                vv = jnp.concatenate(vs, axis=0)
                q = q_s[pl.ds(pl.multiple_of(32 * pair, 32), 32), :].astype(jnp.bfloat16)
                s = lax.dot_general(q, kk, (((1,), (1,)), ((), ())), preferred_element_type=jnp.float32) * scale
                valid = col_pos <= jnp.where(upper, p0, p1)
                s = jnp.where(valid, s, -1e30)
                m = jnp.max(s, axis=1, keepdims=True)
                w = jnp.where(valid, jnp.exp(s - m), 0.0)
                l = jnp.sum(w, axis=1, keepdims=True)
                mix_ref[pair] = jnp.dot(w.astype(jnp.bfloat16), vv, preferred_element_type=jnp.float32)
                m_all = jnp.where(lane == pair, m, m_all)
                l_all = jnp.where(lane == pair, l, l_all)
            m_ref[...] = m_all
            l_ref[...] = l_all
            return carry

        lax.fori_loop(0, RB // 2 // PAIRS, group, 0)
        for cp in store(n):
            cp.start()
        if n >= 1 and n - 1 + RING < blocks:
            for cp in store(n - 1):
                cp.wait()
            for cp in load(n - 1 + RING):
                cp.start()
    for n in range(blocks - RING, blocks):
        for cp in store(n):
            cp.wait()


def attend_call(seq_lens, freq, g_attn, x_tok, wq, wk, wv, k2, v2):
    rows, dim = x_tok.shape
    chunks = (wq.shape[1] + wk.shape[1] + wv.shape[1]) // WN
    batch = k2.shape[0]
    vm = pl.BlockSpec(memory_space=pltpu.VMEM)
    hbm = pl.BlockSpec(memory_space=pl.ANY)
    f32, bf16 = jnp.float32, jnp.bfloat16
    dma = pltpu.SemaphoreType.DMA
    return pl.pallas_call(
        attend_kernel,
        in_specs=[pl.BlockSpec(memory_space=pltpu.SMEM), vm, vm, vm] + [hbm] * 6,
        out_specs=[hbm, hbm, vm, vm, vm],
        out_shape=[
            jax.ShapeDtypeStruct(k2.shape, bf16),
            jax.ShapeDtypeStruct(v2.shape, bf16),
            jax.ShapeDtypeStruct((batch // 2, 32, 128), f32),
            jax.ShapeDtypeStruct((32, 128), f32),
            jax.ShapeDtypeStruct((32, 128), f32),
        ],
        scratch_shapes=[
            pltpu.VMEM((rows, dim), bf16),
            pltpu.VMEM((rows, dim), bf16),
            pltpu.VMEM((chunks, dim, WN), bf16),
            pltpu.VMEM((batch * 16, 128), f32),
            pltpu.VMEM((batch * 8, 128), f32),
            pltpu.VMEM((batch * 8, 128), f32),
            pltpu.VMEM((rows, 128), f32),
            pltpu.VMEM((rows, 128), f32),
            pltpu.VMEM((RING, RB, 128, 128), bf16),
            pltpu.VMEM((RING, RB, 128, 128), bf16),
            dma, dma((chunks,)), dma((RING,)), dma((RING,)), dma((RING,)), dma((RING,)),
        ],
        compiler_params=pltpu.CompilerParams(vmem_limit_bytes=VMEM_LIMIT),
        name="attend",
    )(seq_lens, seq_lens, freq, g_attn, x_tok, wq, wk, wv, k2, v2)


def coords():
    z = lax.axis_index("tp")
    sp = lax.axis_index("sp")
    return z, sp // 4, (sp // 2) % 2, sp % 2


def device(z, y, x, c):
    return (z, y * 4 + x * 2 + c)


def flip(a, on):
    return 1 - a if on else a


def greet(peers):
    barrier = pltpu.get_barrier_semaphore()
    for p in peers:
        pl.semaphore_signal(barrier, inc=1, device_id=p, device_id_type=MESH)
    pl.semaphore_wait(barrier, len(peers))


def remote(src, dst, send, recv, dev):
    return pltpu.make_async_remote_copy(src_ref=src, dst_ref=dst, send_sem=send, recv_sem=recv, device_id=dev, device_id_type=MESH)


def combine_kernel(mix_ref, m_ref, l_ref, o_ref, got1, st_own, st1, comb, stc, got2, st2, s1, r1, s2, r2):
    z, y, x, c = coords()
    partner = device(z, y, x, 1 - c)
    chips = [(y, x), (y, 1 - x), (1 - y, x), (1 - y, 1 - x)]
    greet([partner] + [device(z, b, a, c) for b, a in chips[1:]])

    st_own[0] = m_ref[...]
    st_own[1] = l_ref[...]
    first = []
    for k in (1, 2, 3, 0):
        b, a = chips[k]
        start = 16 * (b * 4 + a * 2 + 1 - c)
        first.append(remote(mix_ref.at[pl.ds(start, 16)], got1.at[k], s1.at[k], r1.at[k], partner))
    stat1 = remote(st_own, st1, s1.at[4], r1.at[4], partner)
    stat1.start()
    for cp in first:
        cp.start()
    stat1.wait_recv()
    ma, mb = st_own[0], st1[0]
    mg = jnp.maximum(ma, mb)
    fa, fb = jnp.exp(ma - mg), jnp.exp(mb - mg)
    stc[0] = mg
    stc[1] = st_own[1] * fa + st1[1] * fb
    second = {}
    stats2 = {}
    for k in (1, 2, 3):
        b, a = chips[k]
        stats2[k] = remote(stc, st2.at[k - 1], s2.at[3 + k - 1], r2.at[3 + k - 1], device(z, b, a, c))
        stats2[k].start()
    for n, k in enumerate((1, 2, 3, 0)):
        b, a = chips[k]
        block = b * 4 + a * 2 + c
        back = (128 - 16 * block) % 128
        ga, gb = pltpu.roll(fa, back, 1), pltpu.roll(fb, back, 1)
        first[n].wait_recv()
        for j in range(16):
            comb[k, j] = mix_ref[16 * block + j] * ga[:, j : j + 1] + got1[k, j] * gb[:, j : j + 1]
        if k:
            second[k] = remote(comb.at[k], got2.at[k - 1], s2.at[k - 1], r2.at[k - 1], device(z, b, a, c))
            second[k].start()
    for k in (1, 2, 3):
        stats2[k].wait_recv()
    ms = [stc[0]] + [st2[k, 0] for k in range(3)]
    ls = [stc[1]] + [st2[k, 1] for k in range(3)]
    mg = jnp.maximum(jnp.maximum(ms[0], ms[1]), jnp.maximum(ms[2], ms[3]))
    fs = [jnp.exp(m - mg) for m in ms]
    total = ls[0] * fs[0] + ls[1] * fs[1] + ls[2] * fs[2] + ls[3] * fs[3]
    block = y * 4 + x * 2 + c
    back = (128 - 16 * block) % 128
    fs = [pltpu.roll(f, back, 1) for f in fs]
    total = pltpu.roll(total, back, 1)
    for k in (1, 2, 3):
        second[k].wait_recv()
    for j in range(16):
        acc = comb[0, j] * fs[0][:, j : j + 1]
        for k in (1, 2, 3):
            acc = acc + got2[k - 1, j] * fs[k][:, j : j + 1]
        o_ref[j] = (acc / total[:, j : j + 1]).astype(jnp.bfloat16)
    for cp in first + [stat1] + [stats2[k] for k in stats2] + [second[k] for k in second]:
        cp.wait_send()


def combine_call(mix, m, l):
    vm = pl.BlockSpec(memory_space=pltpu.VMEM)
    f32 = jnp.float32
    return pl.pallas_call(
        combine_kernel,
        out_shape=jax.ShapeDtypeStruct((16, 32, 128), jnp.bfloat16),
        in_specs=[vm, vm, vm],
        out_specs=vm,
        scratch_shapes=[
            pltpu.VMEM((4, 16, 32, 128), f32),
            pltpu.VMEM((2, 32, 128), f32),
            pltpu.VMEM((2, 32, 128), f32),
            pltpu.VMEM((4, 16, 32, 128), f32),
            pltpu.VMEM((2, 32, 128), f32),
            pltpu.VMEM((3, 16, 32, 128), f32),
            pltpu.VMEM((3, 2, 32, 128), f32),
            pltpu.SemaphoreType.DMA((5,)),
            pltpu.SemaphoreType.DMA((5,)),
            pltpu.SemaphoreType.DMA((6,)),
            pltpu.SemaphoreType.DMA((6,)),
        ],
        compiler_params=pltpu.CompilerParams(collective_id=0, has_side_effects=True, vmem_limit_bytes=VMEM_LIMIT),
        name="combine",
    )(mix, m, l)


def hidden_kernel(part_ref, x_hbm, g_ref, h_ref, hid_ref, x_ref, zb, hbuf, sx, sz, rz, ss, rs, sd, rd):
    z, y, x, c = coords()
    at = pl.multiple_of(32 * (y * 4 + x * 2 + c) + 16 * z, 16)
    cx = pltpu.make_async_copy(x_hbm.at[pl.ds(at, 16)], x_ref, sx)
    cx.start()
    partner = device(z, y, x, 1 - c)
    zdev = device(1 - z, y, x, c)
    z1, x1 = z + c * (1 - 2 * z), x + (1 - c) * (1 - 2 * x)
    z2, x2 = z + (1 - c) * (1 - 2 * z), x + c * (1 - 2 * x)
    dev1, dev2 = device(z1, y, x1, c), device(z2, y, x2, c)
    greet([partner, dev1, dev2])
    cz = remote(part_ref.at[pl.ds(16 * (1 - z), 16)], zb, sz, rz, zdev)
    cz.start()
    cx.wait()
    cz.wait_recv()
    own = part_ref[pl.ds(pl.multiple_of(16 * z, 16), 16), :]
    hid = (x_ref[...].astype(jnp.float32) + (own + zb[...])).astype(jnp.bfloat16).astype(jnp.float32)
    hid_ref[...] = hid
    inv = lax.rsqrt(jnp.mean(hid * hid, axis=-1, keepdims=True) + NORM_EPS)
    slot = lambda zz, xx, cc: (xx * 2 + cc) * 2 + zz
    mine = slot(z, x, c)
    hbuf[mine] = (hid * inv * g_ref[...].astype(jnp.float32).reshape(1, hid.shape[1])).astype(jnp.bfloat16).astype(jnp.float32)

    def send(sl, dev, s, r, n):
        cp = remote(hbuf.at[sl], hbuf.at[sl], s.at[n], r.at[n], dev)
        cp.start()
        return cp

    a1 = send(mine, dev1, ss, rs, 0)
    a2 = send(mine, dev2, ss, rs, 1)
    d0 = send(mine, partner, sd, rd, 0)
    a1.wait_recv()
    s1 = slot(z1, x1, c)
    a3 = send(s1, dev2, ss, rs, 2)
    d1 = send(s1, partner, sd, rd, 1)
    a2.wait_recv()
    d2 = send(slot(z2, x2, c), partner, sd, rd, 2)
    a3.wait_recv()
    d3 = send(slot(1 - z, 1 - x, c), partner, sd, rd, 3)
    for cp in (d0, d1, d2, d3):
        cp.wait_recv()
    for k in range(8):
        h_ref[pl.ds(16 * k, 16), :] = hbuf[k].astype(jnp.bfloat16)
    for cp in (cz, a1, a2, a3, d0, d1, d2, d3):
        cp.wait_send()


def hidden_call(part, x_tok, g):
    vm = pl.BlockSpec(memory_space=pltpu.VMEM)
    f32 = jnp.float32
    dim = part.shape[1]
    dma = pltpu.SemaphoreType.DMA
    return pl.pallas_call(
        hidden_kernel,
        out_shape=[jax.ShapeDtypeStruct((128, dim), jnp.bfloat16), jax.ShapeDtypeStruct((16, dim), f32)],
        in_specs=[vm, pl.BlockSpec(memory_space=pl.ANY), vm],
        out_specs=[vm, vm],
        scratch_shapes=[
            pltpu.VMEM((16, dim), jnp.bfloat16),
            pltpu.VMEM((16, dim), f32),
            pltpu.VMEM((8, 16, dim), f32),
            dma, dma, dma, dma((3,)), dma((3,)), dma((4,)), dma((4,)),
        ],
        compiler_params=pltpu.CompilerParams(collective_id=1, has_side_effects=True, vmem_limit_bytes=VMEM_LIMIT),
        name="hidden",
    )(part, x_tok, g)


def gate_up_kernel(idx_ref, h_ref, wg_ref, wu_ref, m_ref):
    g = jnp.dot(h_ref[...], wg_ref[...], preferred_element_type=jnp.float32).astype(jnp.bfloat16).astype(jnp.float32)
    u = jnp.dot(h_ref[...], wu_ref[...], preferred_element_type=jnp.float32).astype(jnp.bfloat16).astype(jnp.float32)
    m_ref[...] = (jax.nn.silu(g) * u).astype(jnp.bfloat16)


def gate_up_call(idx, h, wg, wu, ways):
    rows, dim = h.shape
    bn = 256
    steps = wg.shape[1] // ways // bn
    wspec = pl.BlockSpec((dim, bn), lambda i, s: (0, s[0] * steps + i))
    return pl.pallas_call(
        gate_up_kernel,
        grid_spec=pltpu.PrefetchScalarGridSpec(
            num_scalar_prefetch=1,
            grid=(steps,),
            in_specs=[pl.BlockSpec((rows, dim), lambda i, s: (0, 0)), wspec, wspec],
            out_specs=pl.BlockSpec((rows, bn), lambda i, s: (0, i)),
        ),
        out_shape=jax.ShapeDtypeStruct((rows, steps * bn), jnp.bfloat16),
        compiler_params=pltpu.CompilerParams(vmem_limit_bytes=VMEM_LIMIT),
        name="gate_up",
    )(idx, h, wg, wu)


def down_kernel(idx_ref, m_ref, wd_ref, o_ref):
    o_ref[...] = jnp.dot(m_ref[...], wd_ref[...], preferred_element_type=jnp.float32)


def down_call(idx, m, wd):
    rows, depth = m.shape
    bn = 512
    return pl.pallas_call(
        down_kernel,
        grid_spec=pltpu.PrefetchScalarGridSpec(
            num_scalar_prefetch=1,
            grid=(wd.shape[1] // bn,),
            in_specs=[pl.BlockSpec((rows, depth), lambda i, s: (0, 0)), pl.BlockSpec((depth, bn), lambda i, s: (s[0], i))],
            out_specs=pl.BlockSpec((rows, bn), lambda i, s: (0, i)),
        ),
        out_shape=jax.ShapeDtypeStruct((rows, wd.shape[1]), jnp.float32),
        compiler_params=pltpu.CompilerParams(vmem_limit_bytes=VMEM_LIMIT),
        name="down",
    )(idx, m, wd)


COLORS = ((0, 1664), (1664, 1664), (3328, 1792))


def output_kernel(part_ref, hid_ref, y_ref, got1, acc, got2, ybuf, s1, r1, s2, r2, sl, rl, sd, rd):
    z, y, x, c = coords()
    partner = device(z, y, x, 1 - c)
    chips = [(z, x), (z, 1 - x), (1 - z, x), (1 - z, 1 - x)]
    near = [device(z, y, 1 - x, c), device(z, 1 - y, x, c), device(1 - z, y, x, c)]
    greet([partner] + near + [device(1 - z, y, 1 - x, c)])
    slot = lambda zz, xx, cc: (xx * 2 + cc) * 2 + zz
    rows16 = lambda s: pl.ds(pl.multiple_of(16 * s, 16), 16)
    order = (3, 1, 2, 0)
    first = {}
    for k in order:
        zz, xx = chips[k]
        first[k] = remote(part_ref.at[rows16(slot(zz, xx, 1 - c))], got1.at[k], s1.at[k], r1.at[k], partner)
        first[k].start()
    second = {}
    for k in order:
        zz, xx = chips[k]
        first[k].wait_recv()
        acc[k] = part_ref[rows16(slot(zz, xx, c)), :] + got1[k]
        if k:
            second[k] = remote(acc.at[k], got2.at[k - 1], s2.at[k - 1], r2.at[k - 1], device(zz, y, xx, c))
            second[k].start()
    for k in (1, 2, 3):
        second[k].wait_recv()
    total = (acc[0] + got2[0]) + (got2[1] + got2[2])
    mine = y * 8 + slot(z, x, c)
    ybuf[mine] = (hid_ref[...] + total).astype(jnp.bfloat16).astype(jnp.float32)

    def shard(mask):
        zz, yy, xx = flip(z, mask & 4), flip(y, mask & 2), flip(x, mask & 1)
        return yy * 8 + slot(zz, xx, c)

    links, locals_ = {}, {}

    def piece(mask, k):
        return ybuf.at[shard(mask), :, pl.ds(*COLORS[k])]

    def push(mask, k, dim):
        n = 7 * k + (mask | (1 << dim)) - 1
        cp = remote(piece(mask, k), piece(mask, k), sl.at[n], rl.at[n], near[dim])
        cp.start()
        links[k, mask | (1 << dim)] = cp

    def across(mask, k):
        n = 8 * k + mask
        cp = remote(piece(mask, k), piece(mask, k), sd.at[n], rd.at[n], partner)
        cp.start()
        locals_[k, mask] = cp

    turn = lambda k: [(k + i) % 3 for i in range(3)]
    for i in range(3):
        for k in range(3):
            push(0, k, turn(k)[i])
    for k in range(3):
        across(0, k)
    for level in ((0,), (1,), (0, 1), (2,), (0, 2), (1, 2), (0, 1, 2)):
        for k in range(3):
            dims = turn(k)
            mask = sum(1 << dims[i] for i in level)
            links[k, mask].wait_recv()
            for i in range(max(level) + 1, 3):
                push(mask, k, dims[i])
            across(mask, k)
    for cp in locals_.values():
        cp.wait_recv()
    for s in range(16):
        y_ref[pl.ds(16 * s, 16), :] = ybuf[s].astype(jnp.bfloat16)
    for cp in list(first.values()) + list(second.values()) + list(links.values()) + list(locals_.values()):
        cp.wait_send()


def output_call(part, hid):
    vm = pl.BlockSpec(memory_space=pltpu.VMEM)
    f32 = jnp.float32
    dim = part.shape[1]
    dma = pltpu.SemaphoreType.DMA
    return pl.pallas_call(
        output_kernel,
        out_shape=jax.ShapeDtypeStruct((256, dim), jnp.bfloat16),
        in_specs=[vm, vm],
        out_specs=vm,
        scratch_shapes=[
            pltpu.VMEM((4, 16, dim), f32),
            pltpu.VMEM((4, 16, dim), f32),
            pltpu.VMEM((3, 16, dim), f32),
            pltpu.VMEM((16, 16, dim), f32),
            dma((4,)), dma((4,)), dma((3,)), dma((3,)), dma((21,)), dma((21,)), dma((24,)), dma((24,)),
        ],
        compiler_params=pltpu.CompilerParams(collective_id=2, has_side_effects=True, vmem_limit_bytes=VMEM_LIMIT),
        name="output",
    )(part, hid)


def solution(mesh):
    cache_spec = P(None, "sp", "tp", None)
    col_spec = P(None, "tp")
    row_spec = P("tp", None)
    full_spec = P()

    def local_step(x_tok, seq_lens, k_blk, v_blk, g_attn, wq_loc, wk_loc, wv_loc, wo_loc, g_mlp, wg_loc, wu_loc, wd_loc):
        batch, seq_blk, kv_loc, head_dim = k_blk.shape
        q_loc = wq_loc.shape[1] // head_dim
        sp = lax.axis_index("sp")
        freq = ROPE_BASE ** (np.arange(head_dim // 2, dtype=np.float64) * (-2.0 / head_dim))
        freq = jnp.asarray(np.concatenate([freq, freq])[None].astype(np.float32))
        flat = (batch, seq_blk * kv_loc, head_dim)
        k_out, v_out, mix, m, l = attend_call(seq_lens, freq, g_attn, x_tok, wq_loc, wk_loc, wv_loc, k_blk.reshape(flat), v_blk.reshape(flat))
        o = combine_call(mix, m, l).reshape(32, q_loc * head_dim)
        part = jnp.dot(o, wo_loc, preferred_element_type=jnp.float32)
        h, hid = hidden_call(part, x_tok, g_mlp)
        idx = (sp % 4).astype(jnp.int32).reshape(1)
        act = gate_up_call(idx, h, wg_loc, wu_loc, 4)
        down = down_call(idx, act, wd_loc)
        y_out = output_call(down, hid)
        return y_out, k_out.reshape(k_blk.shape), v_out.reshape(v_blk.shape)

    return jax.shard_map(local_step, mesh=mesh, in_specs=(full_spec, full_spec, cache_spec, cache_spec, full_spec, col_spec, col_spec, col_spec, row_spec, full_spec, col_spec, col_spec, row_spec), out_specs=(full_spec, cache_spec, cache_spec), check_vma=False)
```

```python
import jax
import jax.numpy as jnp
import numpy as np
from jax import lax
from jax.experimental import pallas as pl
from jax.experimental.pallas import tpu as pltpu
from jax.sharding import PartitionSpec as P

ROPE_BASE = 500000.0
NORM_EPS = 1e-5
MESH = pl.DeviceIdType.MESH
VMEM_LIMIT = 60 * 1024 * 1024
VMEM_MOST = 67043328


WN = 512
RB = 32
RING = 4
AHEAD = 2
PAIRS = 16


def attend_kernel(lens_s, lens_ref, freq_ref, g_ref, x_hbm, wq, wk, wv, kc, vc, ko, vo, mix_ref, m_ref, l_ref,
                  xb, u, wbuf, q_s, kn_s, vn_s, cos_s, sin_s, kbuf, vbuf, sx, sw, sk, sv, tk, tv):
    rows, dim = xb.shape
    nq, nk, nv = wq.shape[1] // WN, wk.shape[1] // WN, wv.shape[1] // WN
    blocks = kc.shape[0] // RB
    base = lax.axis_index("sp") * (kc.shape[1] // 4)

    cx = pltpu.make_async_copy(x_hbm, xb, sx)
    cx.start()

    def weight(w, i, n):
        return pltpu.make_async_copy(w.at[:, pl.ds(pl.multiple_of(i * WN, WN), WN)], wbuf.at[n], sw.at[n])

    chunks = [(wq, i) for i in range(nq)] + [(wk, i) for i in range(nk)] + [(wv, i) for i in range(nv)]
    for n in range(AHEAD):
        weight(*chunks[n], n).start()

    def load(n):
        r, t = pl.ds(n * RB, RB), n % RING
        return pltpu.make_async_copy(kc.at[r], kbuf.at[t], sk.at[t]), pltpu.make_async_copy(vc.at[r], vbuf.at[t], sv.at[t])

    def store(n):
        r, t = pl.ds(n * RB, RB), n % RING
        return pltpu.make_async_copy(kbuf.at[t], ko.at[r], tk.at[t]), pltpu.make_async_copy(vbuf.at[t], vo.at[r], tv.at[t])

    eye = lax.broadcasted_iota(jnp.int32, (rows, rows), 0) == lax.broadcasted_iota(jnp.int32, (rows, rows), 1)
    lens_f = lens_ref[...].astype(jnp.float32).reshape(1, rows)
    pos = jnp.sum(jnp.where(eye, lens_f, 0.0), axis=1, keepdims=True)
    angles = pos * freq_ref[...]
    half = lax.broadcasted_iota(jnp.int32, (rows, 128), 1) < 64
    cos_s[...] = jnp.cos(angles)
    sin_a = jnp.sin(angles)
    sin_s[...] = jnp.where(half, -sin_a, sin_a)
    m_ref[...] = jnp.zeros_like(m_ref)
    l_ref[...] = jnp.zeros_like(l_ref)

    cx.wait()
    gain = g_ref[...].astype(jnp.float32).reshape(1, dim)

    def norm(i, carry):
        r = pl.ds(pl.multiple_of(i * 32, 32), 32)
        xf = xb[r, :].astype(jnp.float32)
        inv = lax.rsqrt(jnp.mean(xf * xf, axis=-1, keepdims=True) + NORM_EPS)
        u[r, :] = (xf * inv * gain).astype(jnp.bfloat16)
        return carry

    lax.fori_loop(0, rows // 32, norm, 0)

    def rope(t):
        return (t * cos_s[...] + pltpu.roll(t, 64, 1) * sin_s[...]).astype(jnp.bfloat16).astype(jnp.float32)

    early = [lambda n=n: weight(*chunks[n], n).start() for n in range(AHEAD, len(chunks))]
    early += [lambda n=n: [cp.start() for cp in load(n)] for n in range(min(RING, blocks))]
    per = WN // 128
    for n, (w, i) in enumerate(chunks):
        weight(w, i, n).wait()
        early.pop(0)()
        y = jnp.dot(u[...], wbuf[n], preferred_element_type=jnp.float32).astype(jnp.bfloat16).astype(jnp.float32)
        for t in range(per):
            head = y[:, t * 128 : (t + 1) * 128]
            head = head if w is wv else rope(head)
            if w is wq:
                q_s[pl.ds(i * per + t, rows, stride=16), :] = head
            else:
                dst = kn_s if w is wk else vn_s
                for again in (0, 4):
                    dst[pl.ds(i * per + t + again, rows, stride=8), :] = head
    for go in early:
        go()

    row_pos = base + lax.broadcasted_iota(jnp.int32, (128, 128), 0) // 4
    ri = lax.broadcasted_iota(jnp.int32, (32, 256), 0)
    ci = lax.broadcasted_iota(jnp.int32, (32, 256), 1)
    same = jnp.logical_and(ri // 16 == ci // 128, (ri % 16) // 4 == ci % 4)
    col_pos = jnp.where(same, base + (ci % 128) // 4, 1 << 30)
    upper = ri < 16
    lane = lax.broadcasted_iota(jnp.int32, (32, 128), 1)
    scale = 128.0 ** -0.5

    for n in range(blocks):
        slot = n % RING
        for cp in load(n):
            cp.wait()

        def group(g, carry, n=n, slot=slot):
            m_all, l_all = m_ref[...], l_ref[...]
            for j in range(PAIRS):
                local = g * PAIRS + j
                pair = n * (RB // 2) + local
                p0 = lens_s[2 * pair]
                p1 = lens_s[2 * pair + 1]
                ks, vs = [], []
                for t, p in ((0, p0), (1, p1)):
                    b = 2 * local + t
                    new = pl.ds(pl.multiple_of(8 * (2 * pair + t), 8), 8)
                    hit = row_pos == p
                    for buf, fresh, acc in ((kbuf, kn_s, ks), (vbuf, vn_s, vs)):
                        old = buf[slot, b].astype(jnp.float32)
                        add = jnp.broadcast_to(fresh[new, :][None], (16, 8, 128)).reshape(128, 128)
                        val = jnp.where(hit, add, old).astype(jnp.bfloat16)
                        buf[slot, b] = val
                        acc.append(val)
                kk = jnp.concatenate(ks, axis=0)
                vv = jnp.concatenate(vs, axis=0)
                q = q_s[pl.ds(pl.multiple_of(32 * pair, 32), 32), :].astype(jnp.bfloat16)
                s = lax.dot_general(q, kk, (((1,), (1,)), ((), ())), preferred_element_type=jnp.float32) * scale
                valid = col_pos <= jnp.where(upper, p0, p1)
                s = jnp.where(valid, s, -1e30)
                m = jnp.max(s, axis=1, keepdims=True)
                w = jnp.where(valid, jnp.exp(s - m), 0.0)
                l = jnp.sum(w, axis=1, keepdims=True)
                mix_ref[pair, :16] = jnp.dot(w[:16, :128].astype(jnp.bfloat16), vs[0], preferred_element_type=jnp.float32)
                mix_ref[pair, 16:] = jnp.dot(w[16:, 128:].astype(jnp.bfloat16), vs[1], preferred_element_type=jnp.float32)
                m_all = jnp.where(lane == pair, m, m_all)
                l_all = jnp.where(lane == pair, l, l_all)
            m_ref[...] = m_all
            l_ref[...] = l_all
            return carry

        lax.fori_loop(0, RB // 2 // PAIRS, group, 0)
        for cp in store(n):
            cp.start()
        if n >= 1 and n - 1 + RING < blocks:
            for cp in store(n - 1):
                cp.wait()
            for cp in load(n - 1 + RING):
                cp.start()
    for n in range(blocks - RING, blocks):
        for cp in store(n):
            cp.wait()


def attend_call(seq_lens, freq, g_attn, x_tok, wq, wk, wv, k2, v2):
    rows, dim = x_tok.shape
    chunks = (wq.shape[1] + wk.shape[1] + wv.shape[1]) // WN
    batch = k2.shape[0]
    vm = pl.BlockSpec(memory_space=pltpu.VMEM)
    hbm = pl.BlockSpec(memory_space=pl.ANY)
    f32, bf16 = jnp.float32, jnp.bfloat16
    dma = pltpu.SemaphoreType.DMA
    return pl.pallas_call(
        attend_kernel,
        in_specs=[pl.BlockSpec(memory_space=pltpu.SMEM), vm, vm, vm] + [hbm] * 6,
        out_specs=[hbm, hbm, vm, vm, vm],
        out_shape=[
            jax.ShapeDtypeStruct(k2.shape, bf16),
            jax.ShapeDtypeStruct(v2.shape, bf16),
            jax.ShapeDtypeStruct((batch // 2, 32, 128), f32),
            jax.ShapeDtypeStruct((32, 128), f32),
            jax.ShapeDtypeStruct((32, 128), f32),
        ],
        scratch_shapes=[
            pltpu.VMEM((rows, dim), bf16),
            pltpu.VMEM((rows, dim), bf16),
            pltpu.VMEM((chunks, dim, WN), bf16),
            pltpu.VMEM((batch * 16, 128), f32),
            pltpu.VMEM((batch * 8, 128), f32),
            pltpu.VMEM((batch * 8, 128), f32),
            pltpu.VMEM((rows, 128), f32),
            pltpu.VMEM((rows, 128), f32),
            pltpu.VMEM((RING, RB, 128, 128), bf16),
            pltpu.VMEM((RING, RB, 128, 128), bf16),
            dma, dma((chunks,)), dma((RING,)), dma((RING,)), dma((RING,)), dma((RING,)),
        ],
        compiler_params=pltpu.CompilerParams(vmem_limit_bytes=VMEM_LIMIT),
        name="attend",
    )(seq_lens, seq_lens, freq, g_attn, x_tok, wq, wk, wv, k2, v2)


def coords():
    z = lax.axis_index("tp")
    sp = lax.axis_index("sp")
    return z, sp // 4, (sp // 2) % 2, sp % 2


def device(z, y, x, c):
    return (z, y * 4 + x * 2 + c)


def flip(a, on):
    return 1 - a if on else a


def greet(peers):
    barrier = pltpu.get_barrier_semaphore()
    for p in peers:
        pl.semaphore_signal(barrier, inc=1, device_id=p, device_id_type=MESH)
    pl.semaphore_wait(barrier, len(peers))


def remote(src, dst, send, recv, dev):
    return pltpu.make_async_remote_copy(src_ref=src, dst_ref=dst, send_sem=send, recv_sem=recv, device_id=dev, device_id_type=MESH)


def combine_kernel(mix_ref, m_ref, l_ref, wo, part_ref, o_s, wbuf, sw, got1, st_own, st1, comb, stc, got2, st2, s1, r1, s2, r2):
    z, y, x, c = coords()
    partner = device(z, y, x, 1 - c)
    chips = [(y, x), (y, 1 - x), (1 - y, x), (1 - y, 1 - x)]
    weights = [pltpu.make_async_copy(wo.at[pl.ds(n * WN, WN)], wbuf.at[pl.ds(n * WN, WN)], sw.at[n]) for n in range(wo.shape[0] // WN)]
    for cp in weights:
        cp.start()
    greet([partner] + [device(z, b, a, c) for b, a in chips[1:]])

    st_own[0] = m_ref[...]
    st_own[1] = l_ref[...]
    first = []
    for k in (1, 2, 3, 0):
        b, a = chips[k]
        start = 16 * (b * 4 + a * 2 + 1 - c)
        first.append(remote(mix_ref.at[pl.ds(start, 16)], got1.at[k], s1.at[k], r1.at[k], partner))
    stat1 = remote(st_own, st1, s1.at[4], r1.at[4], partner)
    stat1.start()
    for cp in first:
        cp.start()
    stat1.wait_recv()
    ma, mb = st_own[0], st1[0]
    mg = jnp.maximum(ma, mb)
    fa, fb = jnp.exp(ma - mg), jnp.exp(mb - mg)
    stc[0] = mg
    stc[1] = st_own[1] * fa + st1[1] * fb
    second = {}
    stats2 = {}
    for k in (1, 2, 3):
        b, a = chips[k]
        stats2[k] = remote(stc, st2.at[k - 1], s2.at[3 + k - 1], r2.at[3 + k - 1], device(z, b, a, c))
        stats2[k].start()
    for n, k in enumerate((1, 2, 3, 0)):
        b, a = chips[k]
        block = b * 4 + a * 2 + c
        back = (128 - 16 * block) % 128
        ga, gb = pltpu.roll(fa, back, 1), pltpu.roll(fb, back, 1)
        first[n].wait_recv()
        for j in range(16):
            comb[k, j] = mix_ref[16 * block + j] * ga[:, j : j + 1] + got1[k, j] * gb[:, j : j + 1]
        if k:
            second[k] = remote(comb.at[k], got2.at[k - 1], s2.at[k - 1], r2.at[k - 1], device(z, b, a, c))
            second[k].start()
    for k in (1, 2, 3):
        stats2[k].wait_recv()
    ms = [stc[0]] + [st2[k, 0] for k in range(3)]
    ls = [stc[1]] + [st2[k, 1] for k in range(3)]
    mg = jnp.maximum(jnp.maximum(ms[0], ms[1]), jnp.maximum(ms[2], ms[3]))
    fs = [jnp.exp(m - mg) for m in ms]
    total = ls[0] * fs[0] + ls[1] * fs[1] + ls[2] * fs[2] + ls[3] * fs[3]
    block = y * 4 + x * 2 + c
    back = (128 - 16 * block) % 128
    fs = [pltpu.roll(f, back, 1) for f in fs]
    total = pltpu.roll(total, back, 1)
    for k in (1, 2, 3):
        second[k].wait_recv()
    for j in range(16):
        acc = comb[0, j] * fs[0][:, j : j + 1]
        for k in (1, 2, 3):
            acc = acc + got2[k - 1, j] * fs[k][:, j : j + 1]
        o_s[32 * j : 32 * j + 32, :] = acc / total[:, j : j + 1]
    o = jnp.concatenate([o_s[pl.ds(h, 32, stride=16), :].astype(jnp.bfloat16) for h in range(16)], axis=1)
    for cp in weights:
        cp.wait()
    for n in range(wo.shape[1] // WN):
        cols = slice(n * WN, (n + 1) * WN)
        part_ref[:, cols] = jnp.dot(o, wbuf[:, cols], preferred_element_type=jnp.float32)
    for cp in first + [stat1] + [stats2[k] for k in stats2] + [second[k] for k in second]:
        cp.wait_send()


def combine_call(mix, m, l, wo):
    vm = pl.BlockSpec(memory_space=pltpu.VMEM)
    f32 = jnp.float32
    depth, dim = wo.shape
    return pl.pallas_call(
        combine_kernel,
        out_shape=jax.ShapeDtypeStruct((32, dim), f32),
        in_specs=[vm, vm, vm, pl.BlockSpec(memory_space=pl.ANY)],
        out_specs=vm,
        scratch_shapes=[
            pltpu.VMEM((512, 128), f32),
            pltpu.VMEM((depth, dim), jnp.bfloat16),
            pltpu.SemaphoreType.DMA((depth // WN,)),
            pltpu.VMEM((4, 16, 32, 128), f32),
            pltpu.VMEM((2, 32, 128), f32),
            pltpu.VMEM((2, 32, 128), f32),
            pltpu.VMEM((4, 16, 32, 128), f32),
            pltpu.VMEM((2, 32, 128), f32),
            pltpu.VMEM((3, 16, 32, 128), f32),
            pltpu.VMEM((3, 2, 32, 128), f32),
            pltpu.SemaphoreType.DMA((5,)),
            pltpu.SemaphoreType.DMA((5,)),
            pltpu.SemaphoreType.DMA((6,)),
            pltpu.SemaphoreType.DMA((6,)),
        ],
        compiler_params=pltpu.CompilerParams(collective_id=0, has_side_effects=True, vmem_limit_bytes=VMEM_LIMIT),
        name="combine",
    )(mix, m, l, wo)


GN = 256
KN = 1024
HELD = 4096


def hidden_kernel(part_ref, x_hbm, g_ref, wg, wu, wd, down_ref, hid_ref, x_ref, zb, hbuf, h_s, act, gbuf, ubuf, dbuf,
                  sg, su, sdw, sx, sz, rz, ss, rs, sd, rd):
    z, y, x, c = coords()
    depth = act.shape[1]
    mine_from = (2 * x + c) * depth
    gates, downs = depth // GN, wd.shape[1] // WN

    def gate_load(w, buf, sem, n):
        r = pl.ds(n * KN, KN)
        return pltpu.make_async_copy(w.at[r, pl.ds(pl.multiple_of(mine_from, GN), depth)], buf.at[r], sem.at[n])

    def down_load(n):
        src = wd.at[pl.ds(pl.multiple_of(mine_from + n * GN, GN), GN), pl.ds(0, dbuf.shape[1])]
        return pltpu.make_async_copy(src, dbuf.at[pl.ds(n * GN, GN)], sdw.at[n])

    at = pl.multiple_of(32 * (y * 4 + x * 2 + c) + 16 * z, 16)
    cx = pltpu.make_async_copy(x_hbm.at[pl.ds(at, 16)], x_ref, sx)
    cx.start()
    loads = [gate_load(w, buf, sem, n) for n in range(wg.shape[0] // KN) for w, buf, sem in ((wg, gbuf, sg), (wu, ubuf, su))]
    loads += [down_load(n) for n in range(gates)]
    for cp in loads:
        cp.start()
    partner = device(z, y, x, 1 - c)
    zdev = device(1 - z, y, x, c)
    z1, x1 = z + c * (1 - 2 * z), x + (1 - c) * (1 - 2 * x)
    z2, x2 = z + (1 - c) * (1 - 2 * z), x + c * (1 - 2 * x)
    dev1, dev2 = device(z1, y, x1, c), device(z2, y, x2, c)
    greet([partner, dev1, dev2])
    cz = remote(part_ref.at[pl.ds(16 * (1 - z), 16)], zb, sz, rz, zdev)
    cz.start()
    cx.wait()
    cz.wait_recv()
    own = part_ref[pl.ds(pl.multiple_of(16 * z, 16), 16), :]
    hid = (x_ref[...].astype(jnp.float32) + (own + zb[...])).astype(jnp.bfloat16).astype(jnp.float32)
    hid_ref[...] = hid
    inv = lax.rsqrt(jnp.mean(hid * hid, axis=-1, keepdims=True) + NORM_EPS)
    slot = lambda zz, xx, cc: (xx * 2 + cc) * 2 + zz
    mine = slot(z, x, c)
    hbuf[mine] = (hid * inv * g_ref[...].astype(jnp.float32).reshape(1, hid.shape[1])).astype(jnp.bfloat16).astype(jnp.float32)

    def send(sl, dev, s, r, n):
        cp = remote(hbuf.at[sl], hbuf.at[sl], s.at[n], r.at[n], dev)
        cp.start()
        return cp

    a1 = send(mine, dev1, ss, rs, 0)
    a2 = send(mine, dev2, ss, rs, 1)
    d0 = send(mine, partner, sd, rd, 0)
    a1.wait_recv()
    s1 = slot(z1, x1, c)
    a3 = send(s1, dev2, ss, rs, 2)
    d1 = send(s1, partner, sd, rd, 1)
    a2.wait_recv()
    d2 = send(slot(z2, x2, c), partner, sd, rd, 2)
    a3.wait_recv()
    d3 = send(slot(1 - z, 1 - x, c), partner, sd, rd, 3)
    for cp in (d0, d1, d2, d3):
        cp.wait_recv()
    for k in range(8):
        h_s[pl.ds(16 * k, 16), :] = hbuf[k].astype(jnp.bfloat16)
    for cp in (cz, a1, a2, a3, d0, d1, d2, d3):
        cp.wait_send()
    up16 = lambda t: t.astype(jnp.bfloat16).astype(jnp.float32)
    for cp in loads[: len(loads) - gates]:
        cp.wait()
    for n in range(gates):
        cols = slice(n * GN, (n + 1) * GN)
        gate = up16(jnp.dot(h_s[...], gbuf[:, cols], preferred_element_type=jnp.float32))
        up = up16(jnp.dot(h_s[...], ubuf[:, cols], preferred_element_type=jnp.float32))
        act[:, cols] = (jax.nn.silu(gate) * up).astype(jnp.bfloat16)
    held = dbuf.shape[1]
    rest = wd.shape[1] - held
    spare = gbuf.at[pl.ds(0, depth), pl.ds(0, rest)]
    last = pltpu.make_async_copy(wd.at[pl.ds(pl.multiple_of(mine_from, GN), depth), pl.ds(held, rest)], spare, sdw.at[gates])
    last.start()
    for cp in loads[len(loads) - gates :]:
        cp.wait()
    for n in range(downs):
        if n * WN == held:
            last.wait()
        wide = dbuf[:, n * WN : (n + 1) * WN] if n * WN < held else gbuf[:depth, n * WN - held : (n + 1) * WN - held]
        down_ref[:, n * WN : (n + 1) * WN] = jnp.dot(act[...], wide, preferred_element_type=jnp.float32)


def hidden_call(part, x_tok, g, wg, wu, wd, ways):
    vm = pl.BlockSpec(memory_space=pltpu.VMEM)
    f32 = jnp.float32
    dim = part.shape[1]
    dma = pltpu.SemaphoreType.DMA
    hbm = pl.BlockSpec(memory_space=pl.ANY)
    depth = wg.shape[1] // ways
    bf16 = jnp.bfloat16
    return pl.pallas_call(
        hidden_kernel,
        out_shape=[jax.ShapeDtypeStruct((128, dim), f32), jax.ShapeDtypeStruct((16, dim), f32)],
        in_specs=[vm, hbm, vm, hbm, hbm, hbm],
        out_specs=[vm, vm],
        scratch_shapes=[
            pltpu.VMEM((16, dim), bf16),
            pltpu.VMEM((16, dim), f32),
            pltpu.VMEM((8, 16, dim), f32),
            pltpu.VMEM((128, dim), bf16),
            pltpu.VMEM((128, depth), bf16),
            pltpu.VMEM((dim, depth), bf16),
            pltpu.VMEM((dim, depth), bf16),
            pltpu.VMEM((depth, HELD), bf16),
            dma((dim // KN,)), dma((dim // KN,)), dma((depth // GN + 1,)),
            dma, dma, dma, dma((3,)), dma((3,)), dma((4,)), dma((4,)),
        ],
        compiler_params=pltpu.CompilerParams(collective_id=1, has_side_effects=True, vmem_limit_bytes=VMEM_MOST),
        name="hidden",
    )(part, x_tok, g, wg, wu, wd)


COLORS = ((0, 1664), (1664, 1664), (3328, 1792))


def output_kernel(part_ref, hid_ref, y_ref, got1, acc, got2, ybuf, s1, r1, s2, r2, sl, rl, sd, rd):
    z, y, x, c = coords()
    partner = device(z, y, x, 1 - c)
    chips = [(z, x), (z, 1 - x), (1 - z, x), (1 - z, 1 - x)]
    near = [device(z, y, 1 - x, c), device(z, 1 - y, x, c), device(1 - z, y, x, c)]
    greet([partner] + near + [device(1 - z, y, 1 - x, c)])
    slot = lambda zz, xx, cc: (xx * 2 + cc) * 2 + zz
    rows16 = lambda s: pl.ds(pl.multiple_of(16 * s, 16), 16)
    order = (3, 1, 2, 0)
    first = {}
    for k in order:
        zz, xx = chips[k]
        first[k] = remote(part_ref.at[rows16(slot(zz, xx, 1 - c))], got1.at[k], s1.at[k], r1.at[k], partner)
        first[k].start()
    second = {}
    for k in order:
        zz, xx = chips[k]
        first[k].wait_recv()
        acc[k] = part_ref[rows16(slot(zz, xx, c)), :] + got1[k]
        if k:
            second[k] = remote(acc.at[k], got2.at[k - 1], s2.at[k - 1], r2.at[k - 1], device(zz, y, xx, c))
            second[k].start()
    for k in (1, 2, 3):
        second[k].wait_recv()
    total = (acc[0] + got2[0]) + (got2[1] + got2[2])
    mine = y * 8 + slot(z, x, c)
    ybuf[mine] = (hid_ref[...] + total).astype(jnp.bfloat16).astype(jnp.float32)

    def shard(mask):
        zz, yy, xx = flip(z, mask & 4), flip(y, mask & 2), flip(x, mask & 1)
        return yy * 8 + slot(zz, xx, c)

    links, locals_ = {}, {}

    def piece(mask, k):
        return ybuf.at[shard(mask), :, pl.ds(*COLORS[k])]

    def push(mask, k, dim):
        n = 7 * k + (mask | (1 << dim)) - 1
        cp = remote(piece(mask, k), piece(mask, k), sl.at[n], rl.at[n], near[dim])
        cp.start()
        links[k, mask | (1 << dim)] = cp

    def across(mask, k):
        n = 8 * k + mask
        cp = remote(piece(mask, k), piece(mask, k), sd.at[n], rd.at[n], partner)
        cp.start()
        locals_[k, mask] = cp

    turn = lambda k: [(k + i) % 3 for i in range(3)]
    for i in range(3):
        for k in range(3):
            push(0, k, turn(k)[i])
    for k in range(3):
        across(0, k)
    for level in ((0,), (1,), (0, 1), (2,), (0, 2), (1, 2), (0, 1, 2)):
        for k in range(3):
            dims = turn(k)
            mask = sum(1 << dims[i] for i in level)
            links[k, mask].wait_recv()
            for i in range(max(level) + 1, 3):
                push(mask, k, dims[i])
            across(mask, k)
    for cp in locals_.values():
        cp.wait_recv()
    for s in range(16):
        y_ref[pl.ds(16 * s, 16), :] = ybuf[s].astype(jnp.bfloat16)
    for cp in list(first.values()) + list(second.values()) + list(links.values()) + list(locals_.values()):
        cp.wait_send()


def output_call(part, hid):
    vm = pl.BlockSpec(memory_space=pltpu.VMEM)
    f32 = jnp.float32
    dim = part.shape[1]
    dma = pltpu.SemaphoreType.DMA
    return pl.pallas_call(
        output_kernel,
        out_shape=jax.ShapeDtypeStruct((256, dim), jnp.bfloat16),
        in_specs=[vm, vm],
        out_specs=vm,
        scratch_shapes=[
            pltpu.VMEM((4, 16, dim), f32),
            pltpu.VMEM((4, 16, dim), f32),
            pltpu.VMEM((3, 16, dim), f32),
            pltpu.VMEM((16, 16, dim), f32),
            dma((4,)), dma((4,)), dma((3,)), dma((3,)), dma((21,)), dma((21,)), dma((24,)), dma((24,)),
        ],
        compiler_params=pltpu.CompilerParams(collective_id=2, has_side_effects=True, vmem_limit_bytes=VMEM_LIMIT),
        name="output",
    )(part, hid)


def solution(mesh):
    cache_spec = P(None, "sp", "tp", None)
    col_spec = P(None, "tp")
    row_spec = P("tp", None)
    full_spec = P()

    def local_step(x_tok, seq_lens, k_blk, v_blk, g_attn, wq_loc, wk_loc, wv_loc, wo_loc, g_mlp, wg_loc, wu_loc, wd_loc):
        batch, seq_blk, kv_loc, head_dim = k_blk.shape
        q_loc = wq_loc.shape[1] // head_dim
        freq = ROPE_BASE ** (np.arange(head_dim // 2, dtype=np.float64) * (-2.0 / head_dim))
        freq = jnp.asarray(np.concatenate([freq, freq])[None].astype(np.float32))
        flat = (batch, seq_blk * kv_loc, head_dim)
        k_out, v_out, mix, m, l = attend_call(seq_lens, freq, g_attn, x_tok, wq_loc, wk_loc, wv_loc, k_blk.reshape(flat), v_blk.reshape(flat))
        part = combine_call(mix, m, l, wo_loc)
        down, hid = hidden_call(part, x_tok, g_mlp, wg_loc, wu_loc, wd_loc, 4)
        y_out = output_call(down, hid)
        return y_out, k_out.reshape(k_blk.shape), v_out.reshape(v_blk.shape)

    return jax.shard_map(local_step, mesh=mesh, in_specs=(full_spec, full_spec, cache_spec, cache_spec, full_spec, col_spec, col_spec, col_spec, row_spec, full_spec, col_spec, col_spec, row_spec), out_specs=(full_spec, cache_spec, cache_spec), check_vma=False)
```

```python
import jax
import jax.numpy as jnp
import numpy as np
from jax import lax
from jax.experimental import pallas as pl
from jax.experimental.pallas import tpu as pltpu
from jax.sharding import PartitionSpec as P

ROPE_BASE = 500000.0
NORM_EPS = 1e-5
MESH = pl.DeviceIdType.MESH
VMEM_LIMIT = 60 * 1024 * 1024
VMEM_MOST = 67043328


WN = 512
RB = 32
RING = 4
AHEAD = 2
PAIRS = 16


def attend_kernel(lens_s, lens_ref, freq_ref, g_ref, x_hbm, wq, wk, wv, kc, vc, ko, vo, mix_ref, m_ref, l_ref,
                  xb, u, wbuf, q_s, kn_s, vn_s, cos_s, sin_s, kbuf, vbuf, sx, sw, sk, sv, tk, tv):
    rows, dim = xb.shape
    nq, nk, nv = wq.shape[1] // WN, wk.shape[1] // WN, wv.shape[1] // WN
    blocks = kc.shape[0] // RB
    base = lax.axis_index("sp") * (kc.shape[1] // 4)

    cx = pltpu.make_async_copy(x_hbm, xb, sx)
    cx.start()

    def weight(w, i, n):
        return pltpu.make_async_copy(w.at[:, pl.ds(pl.multiple_of(i * WN, WN), WN)], wbuf.at[n], sw.at[n])

    chunks = [(wq, i) for i in range(nq)] + [(wk, i) for i in range(nk)] + [(wv, i) for i in range(nv)]
    for n in range(AHEAD):
        weight(*chunks[n], n).start()

    def load(n):
        r, t = pl.ds(n * RB, RB), n % RING
        return pltpu.make_async_copy(kc.at[r], kbuf.at[t], sk.at[t]), pltpu.make_async_copy(vc.at[r], vbuf.at[t], sv.at[t])

    def store(n):
        r, t = pl.ds(n * RB, RB), n % RING
        return pltpu.make_async_copy(kbuf.at[t], ko.at[r], tk.at[t]), pltpu.make_async_copy(vbuf.at[t], vo.at[r], tv.at[t])

    eye = lax.broadcasted_iota(jnp.int32, (rows, rows), 0) == lax.broadcasted_iota(jnp.int32, (rows, rows), 1)
    lens_f = lens_ref[...].astype(jnp.float32).reshape(1, rows)
    pos = jnp.sum(jnp.where(eye, lens_f, 0.0), axis=1, keepdims=True)
    angles = pos * freq_ref[...]
    half = lax.broadcasted_iota(jnp.int32, (rows, 128), 1) < 64
    cos_s[...] = jnp.cos(angles)
    sin_a = jnp.sin(angles)
    sin_s[...] = jnp.where(half, -sin_a, sin_a)
    m_ref[...] = jnp.zeros_like(m_ref)
    l_ref[...] = jnp.zeros_like(l_ref)

    cx.wait()
    gain = g_ref[...].astype(jnp.float32).reshape(1, dim)

    def norm(i, carry):
        r = pl.ds(pl.multiple_of(i * 32, 32), 32)
        xf = xb[r, :].astype(jnp.float32)
        inv = lax.rsqrt(jnp.mean(xf * xf, axis=-1, keepdims=True) + NORM_EPS)
        u[r, :] = (xf * inv * gain).astype(jnp.bfloat16)
        return carry

    lax.fori_loop(0, rows // 32, norm, 0)

    def rope(t):
        return (t * cos_s[...] + pltpu.roll(t, 64, 1) * sin_s[...]).astype(jnp.bfloat16).astype(jnp.float32)

    early = [lambda n=n: weight(*chunks[n], n).start() for n in range(AHEAD, len(chunks))]
    early += [lambda n=n: [cp.start() for cp in load(n)] for n in range(min(RING, blocks))]
    per = WN // 128
    for n, (w, i) in enumerate(chunks):
        weight(w, i, n).wait()
        early.pop(0)()
        y = jnp.dot(u[...], wbuf[n], preferred_element_type=jnp.float32).astype(jnp.bfloat16).astype(jnp.float32)
        for t in range(per):
            head = y[:, t * 128 : (t + 1) * 128]
            head = head if w is wv else rope(head)
            if w is wq:
                q_s[pl.ds(i * per + t, rows, stride=16), :] = head
            else:
                dst = kn_s if w is wk else vn_s
                for again in (0, 4):
                    dst[pl.ds(i * per + t + again, rows, stride=8), :] = head
    for go in early:
        go()

    row_pos = base + lax.broadcasted_iota(jnp.int32, (128, 128), 0) // 4
    ri = lax.broadcasted_iota(jnp.int32, (32, 256), 0)
    ci = lax.broadcasted_iota(jnp.int32, (32, 256), 1)
    same = jnp.logical_and(ri // 16 == ci // 128, (ri % 16) // 4 == ci % 4)
    col_pos = jnp.where(same, base + (ci % 128) // 4, 1 << 30)
    upper = ri < 16
    lane = lax.broadcasted_iota(jnp.int32, (32, 128), 1)
    scale = 128.0 ** -0.5

    for n in range(blocks):
        slot = n % RING
        for cp in load(n):
            cp.wait()

        def group(g, carry, n=n, slot=slot):
            m_all, l_all = m_ref[...], l_ref[...]
            for j in range(PAIRS):
                local = g * PAIRS + j
                pair = n * (RB // 2) + local
                p0 = lens_s[2 * pair]
                p1 = lens_s[2 * pair + 1]
                ks, vs = [], []
                for t, p in ((0, p0), (1, p1)):
                    b = 2 * local + t
                    new = pl.ds(pl.multiple_of(8 * (2 * pair + t), 8), 8)
                    hit = row_pos == p
                    for buf, fresh, acc in ((kbuf, kn_s, ks), (vbuf, vn_s, vs)):
                        old = buf[slot, b].astype(jnp.float32)
                        add = jnp.broadcast_to(fresh[new, :][None], (16, 8, 128)).reshape(128, 128)
                        val = jnp.where(hit, add, old).astype(jnp.bfloat16)
                        buf[slot, b] = val
                        acc.append(val)
                kk = jnp.concatenate(ks, axis=0)
                vv = jnp.concatenate(vs, axis=0)
                q = q_s[pl.ds(pl.multiple_of(32 * pair, 32), 32), :].astype(jnp.bfloat16)
                s = lax.dot_general(q, kk, (((1,), (1,)), ((), ())), preferred_element_type=jnp.float32) * scale
                valid = col_pos <= jnp.where(upper, p0, p1)
                s = jnp.where(valid, s, -1e30)
                m = jnp.max(s, axis=1, keepdims=True)
                w = jnp.where(valid, jnp.exp(s - m), 0.0)
                l = jnp.sum(w, axis=1, keepdims=True)
                mix_ref[pair, :16] = jnp.dot(w[:16, :128].astype(jnp.bfloat16), vs[0], preferred_element_type=jnp.float32)
                mix_ref[pair, 16:] = jnp.dot(w[16:, 128:].astype(jnp.bfloat16), vs[1], preferred_element_type=jnp.float32)
                m_all = jnp.where(lane == pair, m, m_all)
                l_all = jnp.where(lane == pair, l, l_all)
            m_ref[...] = m_all
            l_ref[...] = l_all
            return carry

        lax.fori_loop(0, RB // 2 // PAIRS, group, 0)
        for cp in store(n):
            cp.start()
        if n >= 1 and n - 1 + RING < blocks:
            for cp in store(n - 1):
                cp.wait()
            for cp in load(n - 1 + RING):
                cp.start()
    for n in range(blocks - RING, blocks):
        for cp in store(n):
            cp.wait()


def attend_call(seq_lens, freq, g_attn, x_tok, wq, wk, wv, k2, v2):
    rows, dim = x_tok.shape
    chunks = (wq.shape[1] + wk.shape[1] + wv.shape[1]) // WN
    batch = k2.shape[0]
    vm = pl.BlockSpec(memory_space=pltpu.VMEM)
    hbm = pl.BlockSpec(memory_space=pl.ANY)
    f32, bf16 = jnp.float32, jnp.bfloat16
    dma = pltpu.SemaphoreType.DMA
    return pl.pallas_call(
        attend_kernel,
        in_specs=[pl.BlockSpec(memory_space=pltpu.SMEM), vm, vm, vm] + [hbm] * 6,
        out_specs=[hbm, hbm, vm, vm, vm],
        out_shape=[
            jax.ShapeDtypeStruct(k2.shape, bf16),
            jax.ShapeDtypeStruct(v2.shape, bf16),
            jax.ShapeDtypeStruct((batch // 2, 32, 128), f32),
            jax.ShapeDtypeStruct((32, 128), f32),
            jax.ShapeDtypeStruct((32, 128), f32),
        ],
        scratch_shapes=[
            pltpu.VMEM((rows, dim), bf16),
            pltpu.VMEM((rows, dim), bf16),
            pltpu.VMEM((chunks, dim, WN), bf16),
            pltpu.VMEM((batch * 16, 128), f32),
            pltpu.VMEM((batch * 8, 128), f32),
            pltpu.VMEM((batch * 8, 128), f32),
            pltpu.VMEM((rows, 128), f32),
            pltpu.VMEM((rows, 128), f32),
            pltpu.VMEM((RING, RB, 128, 128), bf16),
            pltpu.VMEM((RING, RB, 128, 128), bf16),
            dma, dma((chunks,)), dma((RING,)), dma((RING,)), dma((RING,)), dma((RING,)),
        ],
        compiler_params=pltpu.CompilerParams(vmem_limit_bytes=VMEM_LIMIT),
        name="attend",
    )(seq_lens, seq_lens, freq, g_attn, x_tok, wq, wk, wv, k2, v2)


def coords():
    z = lax.axis_index("tp")
    sp = lax.axis_index("sp")
    return z, sp // 4, (sp // 2) % 2, sp % 2


def device(z, y, x, c):
    return (z, y * 4 + x * 2 + c)


def flip(a, on):
    return 1 - a if on else a


def greet(peers):
    barrier = pltpu.get_barrier_semaphore()
    for p in peers:
        pl.semaphore_signal(barrier, inc=1, device_id=p, device_id_type=MESH)
    pl.semaphore_wait(barrier, len(peers))


def remote(src, dst, send, recv, dev):
    return pltpu.make_async_remote_copy(src_ref=src, dst_ref=dst, send_sem=send, recv_sem=recv, device_id=dev, device_id_type=MESH)


def combine_kernel(mix_ref, m_ref, l_ref, wo, part_ref, o_s, wbuf, sw, got1, st_own, st1, comb, stc, got2, st2, s1, r1, s2, r2):
    z, y, x, c = coords()
    partner = device(z, y, x, 1 - c)
    chips = [(y, x), (y, 1 - x), (1 - y, x), (1 - y, 1 - x)]
    weights = [pltpu.make_async_copy(wo.at[pl.ds(n * WN, WN)], wbuf.at[pl.ds(n * WN, WN)], sw.at[n]) for n in range(wo.shape[0] // WN)]
    greet([partner] + [device(z, b, a, c) for b, a in chips[1:]])

    st_own[0] = m_ref[...]
    st_own[1] = l_ref[...]
    first = []
    for k in (1, 2, 3, 0):
        b, a = chips[k]
        start = 16 * (b * 4 + a * 2 + 1 - c)
        first.append(remote(mix_ref.at[pl.ds(start, 16)], got1.at[k], s1.at[k], r1.at[k], partner))
    stat1 = remote(st_own, st1, s1.at[4], r1.at[4], partner)
    stat1.start()
    for cp in first:
        cp.start()
    for cp in weights:
        cp.start()
    stat1.wait_recv()
    ma, mb = st_own[0], st1[0]
    mg = jnp.maximum(ma, mb)
    fa, fb = jnp.exp(ma - mg), jnp.exp(mb - mg)
    stc[0] = mg
    stc[1] = st_own[1] * fa + st1[1] * fb
    second = {}
    stats2 = {}
    for k in (1, 2, 3):
        b, a = chips[k]
        stats2[k] = remote(stc, st2.at[k - 1], s2.at[3 + k - 1], r2.at[3 + k - 1], device(z, b, a, c))
        stats2[k].start()
    for n, k in enumerate((1, 2, 3, 0)):
        b, a = chips[k]
        block = b * 4 + a * 2 + c
        back = (128 - 16 * block) % 128
        ga, gb = pltpu.roll(fa, back, 1), pltpu.roll(fb, back, 1)
        first[n].wait_recv()
        for j in range(16):
            comb[k, j] = mix_ref[16 * block + j] * ga[:, j : j + 1] + got1[k, j] * gb[:, j : j + 1]
        if k:
            second[k] = remote(comb.at[k], got2.at[k - 1], s2.at[k - 1], r2.at[k - 1], device(z, b, a, c))
            second[k].start()
    for k in (1, 2, 3):
        stats2[k].wait_recv()
    ms = [stc[0]] + [st2[k, 0] for k in range(3)]
    ls = [stc[1]] + [st2[k, 1] for k in range(3)]
    mg = jnp.maximum(jnp.maximum(ms[0], ms[1]), jnp.maximum(ms[2], ms[3]))
    fs = [jnp.exp(m - mg) for m in ms]
    total = ls[0] * fs[0] + ls[1] * fs[1] + ls[2] * fs[2] + ls[3] * fs[3]
    block = y * 4 + x * 2 + c
    back = (128 - 16 * block) % 128
    fs = [pltpu.roll(f, back, 1) for f in fs]
    total = pltpu.roll(total, back, 1)
    for k in (1, 2, 3):
        second[k].wait_recv()
    for j in range(16):
        acc = comb[0, j] * fs[0][:, j : j + 1]
        for k in (1, 2, 3):
            acc = acc + got2[k - 1, j] * fs[k][:, j : j + 1]
        o_s[32 * j : 32 * j + 32, :] = acc / total[:, j : j + 1]
    o = jnp.concatenate([o_s[pl.ds(h, 32, stride=16), :].astype(jnp.bfloat16) for h in range(16)], axis=1)
    for cp in weights:
        cp.wait()
    for n in range(wo.shape[1] // WN):
        cols = slice(n * WN, (n + 1) * WN)
        part_ref[:, cols] = jnp.dot(o, wbuf[:, cols], preferred_element_type=jnp.float32)
    for cp in first + [stat1] + [stats2[k] for k in stats2] + [second[k] for k in second]:
        cp.wait_send()


def combine_call(mix, m, l, wo):
    vm = pl.BlockSpec(memory_space=pltpu.VMEM)
    f32 = jnp.float32
    depth, dim = wo.shape
    return pl.pallas_call(
        combine_kernel,
        out_shape=jax.ShapeDtypeStruct((32, dim), f32),
        in_specs=[vm, vm, vm, pl.BlockSpec(memory_space=pl.ANY)],
        out_specs=vm,
        scratch_shapes=[
            pltpu.VMEM((512, 128), f32),
            pltpu.VMEM((depth, dim), jnp.bfloat16),
            pltpu.SemaphoreType.DMA((depth // WN,)),
            pltpu.VMEM((4, 16, 32, 128), f32),
            pltpu.VMEM((2, 32, 128), f32),
            pltpu.VMEM((2, 32, 128), f32),
            pltpu.VMEM((4, 16, 32, 128), f32),
            pltpu.VMEM((2, 32, 128), f32),
            pltpu.VMEM((3, 16, 32, 128), f32),
            pltpu.VMEM((3, 2, 32, 128), f32),
            pltpu.SemaphoreType.DMA((5,)),
            pltpu.SemaphoreType.DMA((5,)),
            pltpu.SemaphoreType.DMA((6,)),
            pltpu.SemaphoreType.DMA((6,)),
        ],
        compiler_params=pltpu.CompilerParams(collective_id=0, has_side_effects=True, vmem_limit_bytes=VMEM_LIMIT),
        name="combine",
    )(mix, m, l, wo)


GN = 256
PIECES = 5
KN = 1024
HELD = 4096


def hidden_kernel(part_ref, x_hbm, g_ref, wg, wu, wd, down_ref, hid_ref, x_ref, zb, hbuf, h_s, act, gbuf, ubuf, dbuf,
                  sg, su, sdw, sx, sz, rz, ss, rs, sd, rd):
    z, y, x, c = coords()
    depth = act.shape[1]
    mine_from = (2 * x + c) * depth
    gates, downs = depth // GN, wd.shape[1] // WN

    def gate_load(w, buf, sem, n):
        r = pl.ds(n * KN, KN)
        return pltpu.make_async_copy(w.at[r, pl.ds(pl.multiple_of(mine_from, GN), depth)], buf.at[r], sem.at[n])

    def down_load(n):
        src = wd.at[pl.ds(pl.multiple_of(mine_from + n * GN, GN), GN), pl.ds(0, dbuf.shape[1])]
        return pltpu.make_async_copy(src, dbuf.at[pl.ds(n * GN, GN)], sdw.at[n])

    at = pl.multiple_of(32 * (y * 4 + x * 2 + c) + 16 * z, 16)
    cx = pltpu.make_async_copy(x_hbm.at[pl.ds(at, 16)], x_ref, sx)
    cx.start()
    loads = [gate_load(w, buf, sem, n) for n in range(wg.shape[0] // KN) for w, buf, sem in ((wg, gbuf, sg), (wu, ubuf, su))]
    loads += [down_load(n) for n in range(gates)]
    partner = device(z, y, x, 1 - c)
    zdev = device(1 - z, y, x, c)
    xdev = device(z, y, 1 - x, c)
    dim = zb.shape[1]
    step = dim // PIECES
    cols = [pl.ds(p * step, step) for p in range(PIECES)]
    greet([partner, zdev, xdev])
    sums = [remote(part_ref.at[pl.ds(16 * (1 - z), 16), cols[p]], zb.at[:, cols[p]], sz.at[p], rz.at[p], zdev) for p in range(PIECES)]
    for cp in sums:
        cp.start()
    for cp in loads:
        cp.start()
    cx.wait()
    slot = lambda zz, xx, cc: (xx * 2 + cc) * 2 + zz
    mine = slot(z, x, c)

    def send(sl, p, dev, s, r, n):
        cp = remote(hbuf.at[sl, :, cols[p]], hbuf.at[sl, :, cols[p]], s.at[n * PIECES + p], r.at[n * PIECES + p], dev)
        cp.start()
        return cp

    over_z, over_x, over_c = {}, {}, {}
    for p in range(PIECES):
        sums[p].wait_recv()
        own = part_ref[pl.ds(pl.multiple_of(16 * z, 16), 16), cols[p]] + zb[:, cols[p]]
        hid = (x_ref[:, cols[p]].astype(jnp.float32) + own).astype(jnp.bfloat16).astype(jnp.float32)
        hid_ref[:, cols[p]] = hid
        hbuf[mine, :, cols[p]] = hid
        over_z[p] = send(mine, p, zdev, ss, rs, 0)
        over_x[0, p] = send(mine, p, xdev, ss, rs, 1)
        over_c[0, p] = send(mine, p, partner, sd, rd, 0)
    sz1, sx1, sd1 = slot(1 - z, x, c), slot(z, 1 - x, c), slot(1 - z, 1 - x, c)
    for p in range(PIECES):
        over_z[p].wait_recv()
        over_x[1, p] = send(sz1, p, xdev, ss, rs, 2)
        over_c[1, p] = send(sz1, p, partner, sd, rd, 1)
    gain = g_ref[...].astype(jnp.float32).reshape(1, dim)

    def norm(k):
        hid = hbuf[k]
        inv = lax.rsqrt(jnp.mean(hid * hid, axis=-1, keepdims=True) + NORM_EPS)
        h_s[pl.ds(pl.multiple_of(16 * k, 16), 16), :] = (hid * inv * gain).astype(jnp.bfloat16)

    norm(mine)
    norm(sz1)
    for p in range(PIECES):
        over_x[0, p].wait_recv()
        over_c[2, p] = send(sx1, p, partner, sd, rd, 2)
    for p in range(PIECES):
        over_x[1, p].wait_recv()
        over_c[3, p] = send(sd1, p, partner, sd, rd, 3)
    norm(sx1)
    norm(sd1)
    for n, (zz, xx) in enumerate(((z, x), (1 - z, x), (z, 1 - x), (1 - z, 1 - x))):
        for p in range(PIECES):
            over_c[n, p].wait_recv()
        norm(slot(zz, xx, 1 - c))
    for cp in sums + list(over_z.values()) + list(over_x.values()) + list(over_c.values()):
        cp.wait_send()
    up16 = lambda t: t.astype(jnp.bfloat16).astype(jnp.float32)
    for cp in loads[: len(loads) - gates]:
        cp.wait()
    for n in range(gates):
        part = slice(n * GN, (n + 1) * GN)
        gate = up16(jnp.dot(h_s[...], gbuf[:, part], preferred_element_type=jnp.float32))
        up = up16(jnp.dot(h_s[...], ubuf[:, part], preferred_element_type=jnp.float32))
        act[:, part] = (jax.nn.silu(gate) * up).astype(jnp.bfloat16)
    held = dbuf.shape[1]
    rest = wd.shape[1] - held
    spare = gbuf.at[pl.ds(0, depth), pl.ds(0, rest)]
    last = pltpu.make_async_copy(wd.at[pl.ds(pl.multiple_of(mine_from, GN), depth), pl.ds(held, rest)], spare, sdw.at[gates])
    last.start()
    for cp in loads[len(loads) - gates :]:
        cp.wait()
    for n in range(downs):
        if n * WN == held:
            last.wait()
        wide = dbuf[:, n * WN : (n + 1) * WN] if n * WN < held else gbuf[:depth, n * WN - held : (n + 1) * WN - held]
        down_ref[:, n * WN : (n + 1) * WN] = jnp.dot(act[...], wide, preferred_element_type=jnp.float32)


def hidden_call(part, x_tok, g, wg, wu, wd, ways):
    vm = pl.BlockSpec(memory_space=pltpu.VMEM)
    f32 = jnp.float32
    dim = part.shape[1]
    dma = pltpu.SemaphoreType.DMA
    hbm = pl.BlockSpec(memory_space=pl.ANY)
    depth = wg.shape[1] // ways
    bf16 = jnp.bfloat16
    return pl.pallas_call(
        hidden_kernel,
        out_shape=[jax.ShapeDtypeStruct((128, dim), f32), jax.ShapeDtypeStruct((16, dim), f32)],
        in_specs=[vm, hbm, vm, hbm, hbm, hbm],
        out_specs=[vm, vm],
        scratch_shapes=[
            pltpu.VMEM((16, dim), bf16),
            pltpu.VMEM((16, dim), f32),
            pltpu.VMEM((8, 16, dim), f32),
            pltpu.VMEM((128, dim), bf16),
            pltpu.VMEM((128, depth), bf16),
            pltpu.VMEM((dim, depth), bf16),
            pltpu.VMEM((dim, depth), bf16),
            pltpu.VMEM((depth, HELD), bf16),
            dma((dim // KN,)), dma((dim // KN,)), dma((depth // GN + 1,)),
            dma, dma((PIECES,)), dma((PIECES,)), dma((3 * PIECES,)), dma((3 * PIECES,)), dma((4 * PIECES,)), dma((4 * PIECES,)),
        ],
        compiler_params=pltpu.CompilerParams(collective_id=1, has_side_effects=True, vmem_limit_bytes=VMEM_MOST),
        name="hidden",
    )(part, x_tok, g, wg, wu, wd)


COLORS = ((0, 1664), (1664, 1664), (3328, 1792))


def output_kernel(part_ref, hid_ref, y_ref, got1, acc, got2, ybuf, s1, r1, s2, r2, sl, rl, sd, rd):
    z, y, x, c = coords()
    partner = device(z, y, x, 1 - c)
    chips = [(z, x), (z, 1 - x), (1 - z, x), (1 - z, 1 - x)]
    near = [device(z, y, 1 - x, c), device(z, 1 - y, x, c), device(1 - z, y, x, c)]
    greet([partner] + near + [device(1 - z, y, 1 - x, c)])
    slot = lambda zz, xx, cc: (xx * 2 + cc) * 2 + zz
    rows16 = lambda s: pl.ds(pl.multiple_of(16 * s, 16), 16)
    order = (3, 1, 2, 0)
    first = {}
    for k in order:
        zz, xx = chips[k]
        first[k] = remote(part_ref.at[rows16(slot(zz, xx, 1 - c))], got1.at[k], s1.at[k], r1.at[k], partner)
        first[k].start()
    second = {}
    for k in order:
        zz, xx = chips[k]
        first[k].wait_recv()
        acc[k] = part_ref[rows16(slot(zz, xx, c)), :] + got1[k]
        if k:
            second[k] = remote(acc.at[k], got2.at[k - 1], s2.at[k - 1], r2.at[k - 1], device(zz, y, xx, c))
            second[k].start()
    for k in (1, 2, 3):
        second[k].wait_recv()
    total = (acc[0] + got2[0]) + (got2[1] + got2[2])
    mine = y * 8 + slot(z, x, c)
    ybuf[mine] = (hid_ref[...] + total).astype(jnp.bfloat16).astype(jnp.float32)

    def shard(mask):
        zz, yy, xx = flip(z, mask & 4), flip(y, mask & 2), flip(x, mask & 1)
        return yy * 8 + slot(zz, xx, c)

    links, locals_ = {}, {}

    def piece(mask, k):
        return ybuf.at[shard(mask), :, pl.ds(*COLORS[k])]

    def push(mask, k, dim):
        n = 7 * k + (mask | (1 << dim)) - 1
        cp = remote(piece(mask, k), piece(mask, k), sl.at[n], rl.at[n], near[dim])
        cp.start()
        links[k, mask | (1 << dim)] = cp

    def across(mask, k):
        n = 8 * k + mask
        cp = remote(piece(mask, k), piece(mask, k), sd.at[n], rd.at[n], partner)
        cp.start()
        locals_[k, mask] = cp

    turn = lambda k: [(k + i) % 3 for i in range(3)]
    for i in range(3):
        for k in range(3):
            push(0, k, turn(k)[i])
    for k in range(3):
        across(0, k)
    for level in ((0,), (1,), (0, 1), (2,), (0, 2), (1, 2), (0, 1, 2)):
        for k in range(3):
            dims = turn(k)
            mask = sum(1 << dims[i] for i in level)
            links[k, mask].wait_recv()
            for i in range(max(level) + 1, 3):
                push(mask, k, dims[i])
            across(mask, k)
    for cp in locals_.values():
        cp.wait_recv()
    for s in range(16):
        y_ref[pl.ds(16 * s, 16), :] = ybuf[s].astype(jnp.bfloat16)
    for cp in list(first.values()) + list(second.values()) + list(links.values()) + list(locals_.values()):
        cp.wait_send()


def output_call(part, hid):
    vm = pl.BlockSpec(memory_space=pltpu.VMEM)
    f32 = jnp.float32
    dim = part.shape[1]
    dma = pltpu.SemaphoreType.DMA
    return pl.pallas_call(
        output_kernel,
        out_shape=jax.ShapeDtypeStruct((256, dim), jnp.bfloat16),
        in_specs=[vm, vm],
        out_specs=vm,
        scratch_shapes=[
            pltpu.VMEM((4, 16, dim), f32),
            pltpu.VMEM((4, 16, dim), f32),
            pltpu.VMEM((3, 16, dim), f32),
            pltpu.VMEM((16, 16, dim), f32),
            dma((4,)), dma((4,)), dma((3,)), dma((3,)), dma((21,)), dma((21,)), dma((24,)), dma((24,)),
        ],
        compiler_params=pltpu.CompilerParams(collective_id=2, has_side_effects=True, vmem_limit_bytes=28 * 1024 * 1024),
        name="output",
    )(part, hid)


def solution(mesh):
    cache_spec = P(None, "sp", "tp", None)
    col_spec = P(None, "tp")
    row_spec = P("tp", None)
    full_spec = P()

    def local_step(x_tok, seq_lens, k_blk, v_blk, g_attn, wq_loc, wk_loc, wv_loc, wo_loc, g_mlp, wg_loc, wu_loc, wd_loc):
        batch, seq_blk, kv_loc, head_dim = k_blk.shape
        q_loc = wq_loc.shape[1] // head_dim
        freq = ROPE_BASE ** (np.arange(head_dim // 2, dtype=np.float64) * (-2.0 / head_dim))
        freq = jnp.asarray(np.concatenate([freq, freq])[None].astype(np.float32))
        flat = (batch, seq_blk * kv_loc, head_dim)
        k_out, v_out, mix, m, l = attend_call(seq_lens, freq, g_attn, x_tok, wq_loc, wk_loc, wv_loc, k_blk.reshape(flat), v_blk.reshape(flat))
        part = combine_call(mix, m, l, wo_loc)
        down, hid = hidden_call(part, x_tok, g_mlp, wg_loc, wu_loc, wd_loc, 4)
        y_out = output_call(down, hid)
        return y_out, k_out.reshape(k_blk.shape), v_out.reshape(v_blk.shape)

    return jax.shard_map(local_step, mesh=mesh, in_specs=(full_spec, full_spec, cache_spec, cache_spec, full_spec, col_spec, col_spec, col_spec, row_spec, full_spec, col_spec, col_spec, row_spec), out_specs=(full_spec, cache_spec, cache_spec), check_vma=False)
```

```python
import jax
import jax.numpy as jnp
import numpy as np
from jax import lax
from jax.experimental import pallas as pl
from jax.experimental.pallas import tpu as pltpu
from jax.sharding import PartitionSpec as P

ROPE_BASE = 500000.0
NORM_EPS = 1e-5
MESH = pl.DeviceIdType.MESH
VMEM_LIMIT = 60 * 1024 * 1024
VMEM_MOST = 67043328


WN = 512
RB = 32
RING = 4
AHEAD = 2
PAIRS = 16


def attend_kernel(lens_s, lens_ref, freq_ref, g_ref, x_hbm, wq, wk, wv, kc, vc, ko, vo, mix_ref, m_ref, l_ref,
                  xb, u, wbuf, q_s, kn_s, vn_s, cos_s, sin_s, kbuf, vbuf, sx, sw, sk, sv, tk, tv):
    rows, dim = xb.shape
    nq, nk, nv = wq.shape[1] // WN, wk.shape[1] // WN, wv.shape[1] // WN
    blocks = kc.shape[0] // RB
    base = lax.axis_index("sp") * (kc.shape[1] // 4)

    cx = pltpu.make_async_copy(x_hbm, xb, sx)
    cx.start()

    def weight(w, i, n):
        return pltpu.make_async_copy(w.at[:, pl.ds(pl.multiple_of(i * WN, WN), WN)], wbuf.at[n], sw.at[n])

    chunks = [(wq, i) for i in range(nq)] + [(wk, i) for i in range(nk)] + [(wv, i) for i in range(nv)]
    for n in range(AHEAD):
        weight(*chunks[n], n).start()

    def load(n):
        r, t = pl.ds(n * RB, RB), n % RING
        return pltpu.make_async_copy(kc.at[r], kbuf.at[t], sk.at[t]), pltpu.make_async_copy(vc.at[r], vbuf.at[t], sv.at[t])

    def store(n):
        r, t = pl.ds(n * RB, RB), n % RING
        return pltpu.make_async_copy(kbuf.at[t], ko.at[r], tk.at[t]), pltpu.make_async_copy(vbuf.at[t], vo.at[r], tv.at[t])

    eye = lax.broadcasted_iota(jnp.int32, (rows, rows), 0) == lax.broadcasted_iota(jnp.int32, (rows, rows), 1)
    lens_f = lens_ref[...].astype(jnp.float32).reshape(1, rows)
    pos = jnp.sum(jnp.where(eye, lens_f, 0.0), axis=1, keepdims=True)
    angles = pos * freq_ref[...]
    half = lax.broadcasted_iota(jnp.int32, (rows, 128), 1) < 64
    cos_s[...] = jnp.cos(angles)
    sin_a = jnp.sin(angles)
    sin_s[...] = jnp.where(half, -sin_a, sin_a)
    m_ref[...] = jnp.zeros_like(m_ref)
    l_ref[...] = jnp.zeros_like(l_ref)

    cx.wait()
    gain = g_ref[...].astype(jnp.float32).reshape(1, dim)

    def norm(i, carry):
        r = pl.ds(pl.multiple_of(i * 32, 32), 32)
        xf = xb[r, :].astype(jnp.float32)
        inv = lax.rsqrt(jnp.mean(xf * xf, axis=-1, keepdims=True) + NORM_EPS)
        u[r, :] = (xf * inv * gain).astype(jnp.bfloat16)
        return carry

    lax.fori_loop(0, rows // 32, norm, 0)

    def rope(t):
        return (t * cos_s[...] + pltpu.roll(t, 64, 1) * sin_s[...]).astype(jnp.bfloat16).astype(jnp.float32)

    early = [lambda n=n: weight(*chunks[n], n).start() for n in range(AHEAD, len(chunks))]
    early += [lambda n=n: [cp.start() for cp in load(n)] for n in range(min(RING, blocks))]
    per = WN // 128
    for n, (w, i) in enumerate(chunks):
        weight(w, i, n).wait()
        early.pop(0)()
        y = jnp.dot(u[...], wbuf[n], preferred_element_type=jnp.float32).astype(jnp.bfloat16).astype(jnp.float32)
        for t in range(per):
            head = y[:, t * 128 : (t + 1) * 128]
            head = head if w is wv else rope(head)
            if w is wq:
                q_s[pl.ds(i * per + t, rows, stride=16), :] = head
            else:
                dst = kn_s if w is wk else vn_s
                for again in (0, 4):
                    dst[pl.ds(i * per + t + again, rows, stride=8), :] = head
    for go in early:
        go()

    row_pos = base + lax.broadcasted_iota(jnp.int32, (128, 128), 0) // 4
    ri = lax.broadcasted_iota(jnp.int32, (32, 256), 0)
    ci = lax.broadcasted_iota(jnp.int32, (32, 256), 1)
    same = jnp.logical_and(ri // 16 == ci // 128, (ri % 16) // 4 == ci % 4)
    col_pos = jnp.where(same, base + (ci % 128) // 4, 1 << 30)
    upper = ri < 16
    lane = lax.broadcasted_iota(jnp.int32, (32, 128), 1)
    scale = 128.0 ** -0.5

    for n in range(blocks):
        slot = n % RING
        for cp in load(n):
            cp.wait()

        def group(g, carry, n=n, slot=slot):
            m_all, l_all = m_ref[...], l_ref[...]
            for j in range(PAIRS):
                local = g * PAIRS + j
                pair = n * (RB // 2) + local
                p0 = lens_s[2 * pair]
                p1 = lens_s[2 * pair + 1]
                ks, vs = [], []
                for t, p in ((0, p0), (1, p1)):
                    b = 2 * local + t
                    new = pl.ds(pl.multiple_of(8 * (2 * pair + t), 8), 8)
                    hit = row_pos == p
                    for buf, fresh, acc in ((kbuf, kn_s, ks), (vbuf, vn_s, vs)):
                        old = buf[slot, b].astype(jnp.float32)
                        add = jnp.broadcast_to(fresh[new, :][None], (16, 8, 128)).reshape(128, 128)
                        val = jnp.where(hit, add, old).astype(jnp.bfloat16)
                        buf[slot, b] = val
                        acc.append(val)
                kk = jnp.concatenate(ks, axis=0)
                vv = jnp.concatenate(vs, axis=0)
                q = q_s[pl.ds(pl.multiple_of(32 * pair, 32), 32), :].astype(jnp.bfloat16)
                s = lax.dot_general(q, kk, (((1,), (1,)), ((), ())), preferred_element_type=jnp.float32) * scale
                valid = col_pos <= jnp.where(upper, p0, p1)
                s = jnp.where(valid, s, -1e30)
                m = jnp.max(s, axis=1, keepdims=True)
                w = jnp.where(valid, jnp.exp(s - m), 0.0)
                l = jnp.sum(w, axis=1, keepdims=True)
                mix_ref[pair, :16] = jnp.dot(w[:16, :128].astype(jnp.bfloat16), vs[0], preferred_element_type=jnp.float32)
                mix_ref[pair, 16:] = jnp.dot(w[16:, 128:].astype(jnp.bfloat16), vs[1], preferred_element_type=jnp.float32)
                m_all = jnp.where(lane == pair, m, m_all)
                l_all = jnp.where(lane == pair, l, l_all)
            m_ref[...] = m_all
            l_ref[...] = l_all
            return carry

        lax.fori_loop(0, RB // 2 // PAIRS, group, 0)
        for cp in store(n):
            cp.start()
        if n >= 1 and n - 1 + RING < blocks:
            for cp in store(n - 1):
                cp.wait()
            for cp in load(n - 1 + RING):
                cp.start()
    for n in range(blocks - RING, blocks):
        for cp in store(n):
            cp.wait()


def attend_call(seq_lens, freq, g_attn, x_tok, wq, wk, wv, k2, v2):
    rows, dim = x_tok.shape
    chunks = (wq.shape[1] + wk.shape[1] + wv.shape[1]) // WN
    batch = k2.shape[0]
    vm = pl.BlockSpec(memory_space=pltpu.VMEM)
    hbm = pl.BlockSpec(memory_space=pl.ANY)
    f32, bf16 = jnp.float32, jnp.bfloat16
    dma = pltpu.SemaphoreType.DMA
    return pl.pallas_call(
        attend_kernel,
        in_specs=[pl.BlockSpec(memory_space=pltpu.SMEM), vm, vm, vm] + [hbm] * 6,
        out_specs=[hbm, hbm, vm, vm, vm],
        out_shape=[
            jax.ShapeDtypeStruct(k2.shape, bf16),
            jax.ShapeDtypeStruct(v2.shape, bf16),
            jax.ShapeDtypeStruct((batch // 2, 32, 128), f32),
            jax.ShapeDtypeStruct((32, 128), f32),
            jax.ShapeDtypeStruct((32, 128), f32),
        ],
        scratch_shapes=[
            pltpu.VMEM((rows, dim), bf16),
            pltpu.VMEM((rows, dim), bf16),
            pltpu.VMEM((chunks, dim, WN), bf16),
            pltpu.VMEM((batch * 16, 128), f32),
            pltpu.VMEM((batch * 8, 128), f32),
            pltpu.VMEM((batch * 8, 128), f32),
            pltpu.VMEM((rows, 128), f32),
            pltpu.VMEM((rows, 128), f32),
            pltpu.VMEM((RING, RB, 128, 128), bf16),
            pltpu.VMEM((RING, RB, 128, 128), bf16),
            dma, dma((chunks,)), dma((RING,)), dma((RING,)), dma((RING,)), dma((RING,)),
        ],
        compiler_params=pltpu.CompilerParams(vmem_limit_bytes=VMEM_LIMIT),
        name="attend",
    )(seq_lens, seq_lens, freq, g_attn, x_tok, wq, wk, wv, k2, v2)


def coords():
    z = lax.axis_index("tp")
    sp = lax.axis_index("sp")
    return z, sp // 4, (sp // 2) % 2, sp % 2


def device(z, y, x, c):
    return (z, y * 4 + x * 2 + c)


def flip(a, on):
    return 1 - a if on else a


def greet(peers):
    barrier = pltpu.get_barrier_semaphore()
    for p in peers:
        pl.semaphore_signal(barrier, inc=1, device_id=p, device_id_type=MESH)
    pl.semaphore_wait(barrier, len(peers))


def remote(src, dst, send, recv, dev):
    return pltpu.make_async_remote_copy(src_ref=src, dst_ref=dst, send_sem=send, recv_sem=recv, device_id=dev, device_id_type=MESH)


def combine_kernel(mix_ref, m_ref, l_ref, wo, part_ref, o_s, wbuf, sw, got1, st_own, st1, comb, stc, stn, got2, st2, s1, r1, s2, r2):
    z, y, x, c = coords()
    partner = device(z, y, x, 1 - c)
    chips = [(y, x), (y, 1 - x), (1 - y, x), (1 - y, 1 - x)]
    y1, x1 = y + c * (1 - 2 * y), x + (1 - c) * (1 - 2 * x)
    y2, x2 = y + (1 - c) * (1 - 2 * y), x + c * (1 - 2 * x)
    dev1, dev2 = device(z, y1, x1, c), device(z, y2, x2, c)
    k1, k2 = 1 + c, 2 - c
    greet([partner, dev1, dev2])

    st_own[0] = m_ref[...]
    st_own[1] = l_ref[...]
    stat1 = remote(st_own, st1, s1.at[4], r1.at[4], partner)
    stat1.start()
    first = {}
    for k in (3, 1, 2, 0):
        b, a = chips[k]
        start = 16 * (b * 4 + a * 2 + 1 - c)
        first[k] = remote(mix_ref.at[pl.ds(start, 16)], got1.at[k], s1.at[k], r1.at[k], partner)
        first[k].start()
    weights = [pltpu.make_async_copy(wo.at[pl.ds(n * WN, WN)], wbuf.at[pl.ds(n * WN, WN)], sw.at[n]) for n in range(wo.shape[0] // WN)]

    def merge(pa, pb):
        m = jnp.maximum(pa[0], pb[0])
        fa, fb = jnp.exp(pa[0] - m), jnp.exp(pb[0] - m)
        return m, pa[1] * fa + pb[1] * fb, fa, fb

    def turned(f, b, a):
        return pltpu.roll(f, (128 - 16 * (b * 4 + a * 2 + c)) % 128, 1)

    stat1.wait_recv()
    m, l, fa, fb = merge((st_own[0], st_own[1]), (st1[0], st1[1]))
    stc[0] = m
    stc[1] = l
    stat2 = remote(stc, st2.at[0], s2.at[3], r2.at[3], dev1)
    stat2.start()

    def pair_sum(k):
        b, a = chips[k]
        ga, gb = turned(fa, b, a), turned(fb, b, a)
        first[k].wait_recv()
        for j in range(16):
            comb[k, j] = mix_ref[16 * (b * 4 + a * 2 + c) + j] * ga[:, j : j + 1] + got1[k, j] * gb[:, j : j + 1]

    def hop(src, dst, dev):
        cp = remote(comb.at[src], got2.at[dst], s2.at[dst], r2.at[dst], dev)
        cp.start()
        return cp

    pair_sum(3)
    far = hop(3, 0, dev1)
    pair_sum(1)
    pair_sum(2)
    direct = hop(k1, 1, dev1)
    for cp in weights:
        cp.start()
    pair_sum(0)
    stat2.wait_recv()
    m, l, fa, fb = merge((m, l), (st2[0, 0], st2[0, 1]))
    stn[0] = m
    stn[1] = l
    stat3 = remote(stn, st2.at[1], s2.at[4], r2.at[4], dev2)
    stat3.start()
    ga, gb = turned(fa, y2, x2), turned(fb, y2, x2)
    far.wait_recv()
    for j in range(16):
        comb[4, j] = comb[k2, j] * ga[:, j : j + 1] + got2[0, j] * gb[:, j : j + 1]
    second = hop(4, 2, dev2)
    stat3.wait_recv()
    _, l, na, nb = merge((m, l), (st2[1, 0], st2[1, 1]))
    fa, fb, nb, l = turned(fa * na, y, x), turned(fb * na, y, x), turned(nb, y, x), turned(l, y, x)
    direct.wait_recv()
    second.wait_recv()
    for j in range(16):
        at = slice(j, j + 1)
        acc = comb[0, j] * fa[:, at] + got2[1, j] * fb[:, at] + got2[2, j] * nb[:, at]
        o_s[32 * j : 32 * j + 32, :] = acc / l[:, at]
    o = jnp.concatenate([o_s[pl.ds(h, 32, stride=16), :].astype(jnp.bfloat16) for h in range(16)], axis=1)
    for cp in weights:
        cp.wait()
    for n in range(wo.shape[1] // WN):
        cols = slice(n * WN, (n + 1) * WN)
        part_ref[:, cols] = jnp.dot(o, wbuf[:, cols], preferred_element_type=jnp.float32)
    for cp in list(first.values()) + [stat1, stat2, stat3, far, direct, second]:
        cp.wait_send()


def combine_call(mix, m, l, wo):
    vm = pl.BlockSpec(memory_space=pltpu.VMEM)
    f32 = jnp.float32
    depth, dim = wo.shape
    return pl.pallas_call(
        combine_kernel,
        out_shape=jax.ShapeDtypeStruct((32, dim), f32),
        in_specs=[vm, vm, vm, pl.BlockSpec(memory_space=pl.ANY)],
        out_specs=vm,
        scratch_shapes=[
            pltpu.VMEM((512, 128), f32),
            pltpu.VMEM((depth, dim), jnp.bfloat16),
            pltpu.SemaphoreType.DMA((depth // WN,)),
            pltpu.VMEM((4, 16, 32, 128), f32),
            pltpu.VMEM((2, 32, 128), f32),
            pltpu.VMEM((2, 32, 128), f32),
            pltpu.VMEM((5, 16, 32, 128), f32),
            pltpu.VMEM((2, 32, 128), f32),
            pltpu.VMEM((2, 32, 128), f32),
            pltpu.VMEM((3, 16, 32, 128), f32),
            pltpu.VMEM((2, 2, 32, 128), f32),
            pltpu.SemaphoreType.DMA((5,)),
            pltpu.SemaphoreType.DMA((5,)),
            pltpu.SemaphoreType.DMA((5,)),
            pltpu.SemaphoreType.DMA((5,)),
        ],
        compiler_params=pltpu.CompilerParams(collective_id=0, has_side_effects=True, vmem_limit_bytes=VMEM_LIMIT),
        name="combine",
    )(mix, m, l, wo)


GN = 256
PIECES = 5
KN = 1024
HELD = 4096


def hidden_kernel(part_ref, x_hbm, g_ref, wg, wu, wd, down_ref, hid_ref, x_ref, zb, hbuf, h_s, act, gbuf, ubuf, dbuf,
                  sg, su, sdw, sx, sz, rz, ss, rs, sd, rd):
    z, y, x, c = coords()
    depth = act.shape[1]
    mine_from = (2 * x + c) * depth
    gates, downs = depth // GN, wd.shape[1] // WN

    def gate_load(w, buf, sem, n):
        r = pl.ds(n * KN, KN)
        return pltpu.make_async_copy(w.at[r, pl.ds(pl.multiple_of(mine_from, GN), depth)], buf.at[r], sem.at[n])

    def down_load(n):
        src = wd.at[pl.ds(pl.multiple_of(mine_from + n * GN, GN), GN), pl.ds(0, dbuf.shape[1])]
        return pltpu.make_async_copy(src, dbuf.at[pl.ds(n * GN, GN)], sdw.at[n])

    at = pl.multiple_of(32 * (y * 4 + x * 2 + c) + 16 * z, 16)
    cx = pltpu.make_async_copy(x_hbm.at[pl.ds(at, 16)], x_ref, sx)
    cx.start()
    loads = [gate_load(w, buf, sem, n) for n in range(wg.shape[0] // KN) for w, buf, sem in ((wg, gbuf, sg), (wu, ubuf, su))]
    loads += [down_load(n) for n in range(gates)]
    partner = device(z, y, x, 1 - c)
    zdev = device(1 - z, y, x, c)
    xdev = device(z, y, 1 - x, c)
    dim = zb.shape[1]
    step = dim // PIECES
    cols = [pl.ds(p * step, step) for p in range(PIECES)]
    greet([partner, zdev, xdev])
    sums = [remote(part_ref.at[pl.ds(16 * (1 - z), 16), cols[p]], zb.at[:, cols[p]], sz.at[p], rz.at[p], zdev) for p in range(PIECES)]
    for cp in sums:
        cp.start()
    for cp in loads:
        cp.start()
    cx.wait()
    slot = lambda zz, xx, cc: (xx * 2 + cc) * 2 + zz
    mine = slot(z, x, c)

    def send(sl, p, dev, s, r, n):
        cp = remote(hbuf.at[sl, :, cols[p]], hbuf.at[sl, :, cols[p]], s.at[n * PIECES + p], r.at[n * PIECES + p], dev)
        cp.start()
        return cp

    over_z, over_x, over_c = {}, {}, {}
    for p in range(PIECES):
        sums[p].wait_recv()
        own = part_ref[pl.ds(pl.multiple_of(16 * z, 16), 16), cols[p]] + zb[:, cols[p]]
        hid = (x_ref[:, cols[p]].astype(jnp.float32) + own).astype(jnp.bfloat16).astype(jnp.float32)
        hid_ref[:, cols[p]] = hid
        hbuf[mine, :, cols[p]] = hid
        over_z[p] = send(mine, p, zdev, ss, rs, 0)
        over_x[0, p] = send(mine, p, xdev, ss, rs, 1)
        over_c[0, p] = send(mine, p, partner, sd, rd, 0)
    sz1, sx1, sd1 = slot(1 - z, x, c), slot(z, 1 - x, c), slot(1 - z, 1 - x, c)
    for p in range(PIECES):
        over_z[p].wait_recv()
        over_x[1, p] = send(sz1, p, xdev, ss, rs, 2)
        over_c[1, p] = send(sz1, p, partner, sd, rd, 1)
    gain = g_ref[...].astype(jnp.float32).reshape(1, dim)

    def norm(k):
        hid = hbuf[k]
        inv = lax.rsqrt(jnp.mean(hid * hid, axis=-1, keepdims=True) + NORM_EPS)
        h_s[pl.ds(pl.multiple_of(16 * k, 16), 16), :] = (hid * inv * gain).astype(jnp.bfloat16)

    norm(mine)
    norm(sz1)
    for p in range(PIECES):
        over_x[0, p].wait_recv()
        over_c[2, p] = send(sx1, p, partner, sd, rd, 2)
    for p in range(PIECES):
        over_x[1, p].wait_recv()
        over_c[3, p] = send(sd1, p, partner, sd, rd, 3)
    norm(sx1)
    norm(sd1)
    for n, (zz, xx) in enumerate(((z, x), (1 - z, x), (z, 1 - x), (1 - z, 1 - x))):
        for p in range(PIECES):
            over_c[n, p].wait_recv()
        norm(slot(zz, xx, 1 - c))
    for cp in sums + list(over_z.values()) + list(over_x.values()) + list(over_c.values()):
        cp.wait_send()
    up16 = lambda t: t.astype(jnp.bfloat16).astype(jnp.float32)
    for cp in loads[: len(loads) - gates]:
        cp.wait()
    for n in range(gates):
        part = slice(n * GN, (n + 1) * GN)
        gate = up16(jnp.dot(h_s[...], gbuf[:, part], preferred_element_type=jnp.float32))
        up = up16(jnp.dot(h_s[...], ubuf[:, part], preferred_element_type=jnp.float32))
        act[:, part] = (jax.nn.silu(gate) * up).astype(jnp.bfloat16)
    held = dbuf.shape[1]
    rest = wd.shape[1] - held
    spare = gbuf.at[pl.ds(0, depth), pl.ds(0, rest)]
    last = pltpu.make_async_copy(wd.at[pl.ds(pl.multiple_of(mine_from, GN), depth), pl.ds(held, rest)], spare, sdw.at[gates])
    last.start()
    for cp in loads[len(loads) - gates :]:
        cp.wait()
    for n in range(downs):
        if n * WN == held:
            last.wait()
        wide = dbuf[:, n * WN : (n + 1) * WN] if n * WN < held else gbuf[:depth, n * WN - held : (n + 1) * WN - held]
        down_ref[:, n * WN : (n + 1) * WN] = jnp.dot(act[...], wide, preferred_element_type=jnp.float32)


def hidden_call(part, x_tok, g, wg, wu, wd, ways):
    vm = pl.BlockSpec(memory_space=pltpu.VMEM)
    f32 = jnp.float32
    dim = part.shape[1]
    dma = pltpu.SemaphoreType.DMA
    hbm = pl.BlockSpec(memory_space=pl.ANY)
    depth = wg.shape[1] // ways
    bf16 = jnp.bfloat16
    return pl.pallas_call(
        hidden_kernel,
        out_shape=[jax.ShapeDtypeStruct((128, dim), f32), jax.ShapeDtypeStruct((16, dim), f32)],
        in_specs=[vm, hbm, vm, hbm, hbm, hbm],
        out_specs=[vm, vm],
        scratch_shapes=[
            pltpu.VMEM((16, dim), bf16),
            pltpu.VMEM((16, dim), f32),
            pltpu.VMEM((8, 16, dim), f32),
            pltpu.VMEM((128, dim), bf16),
            pltpu.VMEM((128, depth), bf16),
            pltpu.VMEM((dim, depth), bf16),
            pltpu.VMEM((dim, depth), bf16),
            pltpu.VMEM((depth, HELD), bf16),
            dma((dim // KN,)), dma((dim // KN,)), dma((depth // GN + 1,)),
            dma, dma((PIECES,)), dma((PIECES,)), dma((3 * PIECES,)), dma((3 * PIECES,)), dma((4 * PIECES,)), dma((4 * PIECES,)),
        ],
        compiler_params=pltpu.CompilerParams(collective_id=1, has_side_effects=True, vmem_limit_bytes=VMEM_MOST),
        name="hidden",
    )(part, x_tok, g, wg, wu, wd)


COLORS = ((0, 1664), (1664, 1664), (3328, 1792))


def output_kernel(part_ref, hid_ref, y_ref, got1, acc, got2, ybuf, s1, r1, s2, r2, sl, rl, sd, rd):
    z, y, x, c = coords()
    partner = device(z, y, x, 1 - c)
    chips = [(z, x), (z, 1 - x), (1 - z, x), (1 - z, 1 - x)]
    near = [device(z, y, 1 - x, c), device(z, 1 - y, x, c), device(1 - z, y, x, c)]
    greet([partner] + near)
    slot = lambda zz, xx, cc: (xx * 2 + cc) * 2 + zz
    rows16 = lambda s: pl.ds(pl.multiple_of(16 * s, 16), 16)
    cols = [pl.ds(*color) for color in COLORS]
    z1, x1 = z + c * (1 - 2 * z), x + (1 - c) * (1 - 2 * x)
    z2, x2 = z + (1 - c) * (1 - 2 * z), x + c * (1 - 2 * x)
    dev1, dev2 = device(z1, y, x1, c), device(z2, y, x2, c)
    k1, k2 = 1 + c, 2 - c
    links, locals_, sums = {}, {}, []
    first = {}
    for p in range(3):
        for k in (3, 1, 2, 0):
            zz, xx = chips[k]
            n = 4 * p + k
            first[k, p] = remote(part_ref.at[rows16(slot(zz, xx, 1 - c)), cols[p]], got1.at[k, :, cols[p]], s1.at[n], r1.at[n], partner)
            first[k, p].start()

    def hop(src, dst, p, dev):
        n = 3 * p + dst
        cp = remote(acc.at[src, :, cols[p]], got2.at[dst, :, cols[p]], s2.at[n], r2.at[n], dev)
        cp.start()
        sums.append(cp)
        return cp

    far, direct, second = {}, {}, {}
    for p in range(3):
        for k in (3, 1, 2, 0):
            zz, xx = chips[k]
            first[k, p].wait_recv()
            acc[k, :, cols[p]] = part_ref[rows16(slot(zz, xx, c)), cols[p]] + got1[k, :, cols[p]]
        far[p] = hop(3, 0, p, dev1)
        direct[p] = hop(k1, 1, p, dev1)
    for p in range(3):
        far[p].wait_recv()
        acc[4, :, cols[p]] = acc[k2, :, cols[p]] + got2[0, :, cols[p]]
        second[p] = hop(4, 2, p, dev2)
    mine = y * 8 + slot(z, x, c)

    def shard(mask):
        zz, yy, xx = flip(z, mask & 4), flip(y, mask & 2), flip(x, mask & 1)
        return yy * 8 + slot(zz, xx, c)

    def piece(mask, k):
        return ybuf.at[shard(mask), :, pl.ds(*COLORS[k])]

    def push(mask, k, dim):
        n = 7 * k + (mask | (1 << dim)) - 1
        cp = remote(piece(mask, k), piece(mask, k), sl.at[n], rl.at[n], near[dim])
        cp.start()
        links[k, mask | (1 << dim)] = cp

    def across(mask, k):
        n = 8 * k + mask
        cp = remote(piece(mask, k), piece(mask, k), sd.at[n], rd.at[n], partner)
        cp.start()
        locals_[k, mask] = cp

    turn = lambda k: [(k + i) % 3 for i in range(3)]
    for k in range(3):
        direct[k].wait_recv()
        near_sum = acc[0, :, cols[k]] + got2[1, :, cols[k]]
        second[k].wait_recv()
        total = near_sum + got2[2, :, cols[k]]
        ybuf[mine, :, cols[k]] = (hid_ref[:, cols[k]] + total).astype(jnp.bfloat16).astype(jnp.float32)
        for i in range(3):
            push(0, k, turn(k)[i])
        across(0, k)
    for level in ((0,), (1,), (0, 1), (2,), (0, 2), (1, 2), (0, 1, 2)):
        for k in range(3):
            dims = turn(k)
            mask = sum(1 << dims[i] for i in level)
            links[k, mask].wait_recv()
            for i in range(max(level) + 1, 3):
                push(mask, k, dims[i])
            across(mask, k)
    for cp in locals_.values():
        cp.wait_recv()
    for s in range(16):
        y_ref[pl.ds(16 * s, 16), :] = ybuf[s].astype(jnp.bfloat16)
    for cp in list(first.values()) + sums + list(links.values()) + list(locals_.values()):
        cp.wait_send()


def output_call(part, hid):
    vm = pl.BlockSpec(memory_space=pltpu.VMEM)
    f32 = jnp.float32
    dim = part.shape[1]
    dma = pltpu.SemaphoreType.DMA
    return pl.pallas_call(
        output_kernel,
        out_shape=jax.ShapeDtypeStruct((256, dim), jnp.bfloat16),
        in_specs=[vm, vm],
        out_specs=vm,
        scratch_shapes=[
            pltpu.VMEM((4, 16, dim), f32),
            pltpu.VMEM((5, 16, dim), f32),
            pltpu.VMEM((3, 16, dim), f32),
            pltpu.VMEM((16, 16, dim), f32),
            dma((12,)), dma((12,)), dma((9,)), dma((9,)), dma((21,)), dma((21,)), dma((24,)), dma((24,)),
        ],
        compiler_params=pltpu.CompilerParams(collective_id=2, has_side_effects=True, vmem_limit_bytes=28 * 1024 * 1024),
        name="output",
    )(part, hid)


def solution(mesh):
    cache_spec = P(None, "sp", "tp", None)
    col_spec = P(None, "tp")
    row_spec = P("tp", None)
    full_spec = P()

    def local_step(x_tok, seq_lens, k_blk, v_blk, g_attn, wq_loc, wk_loc, wv_loc, wo_loc, g_mlp, wg_loc, wu_loc, wd_loc):
        batch, seq_blk, kv_loc, head_dim = k_blk.shape
        q_loc = wq_loc.shape[1] // head_dim
        freq = ROPE_BASE ** (np.arange(head_dim // 2, dtype=np.float64) * (-2.0 / head_dim))
        freq = jnp.asarray(np.concatenate([freq, freq])[None].astype(np.float32))
        flat = (batch, seq_blk * kv_loc, head_dim)
        k_out, v_out, mix, m, l = attend_call(seq_lens, freq, g_attn, x_tok, wq_loc, wk_loc, wv_loc, k_blk.reshape(flat), v_blk.reshape(flat))
        part = combine_call(mix, m, l, wo_loc)
        down, hid = hidden_call(part, x_tok, g_mlp, wg_loc, wu_loc, wd_loc, 4)
        y_out = output_call(down, hid)
        return y_out, k_out.reshape(k_blk.shape), v_out.reshape(v_blk.shape)

    return jax.shard_map(local_step, mesh=mesh, in_specs=(full_spec, full_spec, cache_spec, cache_spec, full_spec, col_spec, col_spec, col_spec, row_spec, full_spec, col_spec, col_spec, row_spec), out_specs=(full_spec, cache_spec, cache_spec), check_vma=False)
```

```python
import jax
import jax.numpy as jnp
import numpy as np
from jax import lax
from jax.experimental import pallas as pl
from jax.experimental.pallas import tpu as pltpu
from jax.sharding import PartitionSpec as P

ROPE_BASE = 500000.0
NORM_EPS = 1e-5
MESH = pl.DeviceIdType.MESH
VMEM_LIMIT = 60 * 1024 * 1024
VMEM_MOST = 67043328


WN = 512
RB = 32
RING = 4
AHEAD = 2
PAIRS = 16


def attend_kernel(lens_s, lens_ref, freq_ref, g_ref, x_hbm, wq, wk, wv, kc, vc, ko, vo, mix_out, st_ref,
                  mix_ref, smix, xb, u, wbuf, q_s, kn_s, vn_s, cos_s, sin_s, kbuf, vbuf, sx, sw, sk, sv, tk, tv):
    rows, dim = xb.shape
    nq, nk, nv = wq.shape[1] // WN, wk.shape[1] // WN, wv.shape[1] // WN
    blocks = kc.shape[0] // RB
    base = lax.axis_index("sp") * (kc.shape[1] // 4)

    cx = pltpu.make_async_copy(x_hbm, xb, sx)
    cx.start()

    def weight(w, i, n):
        return pltpu.make_async_copy(w.at[:, pl.ds(pl.multiple_of(i * WN, WN), WN)], wbuf.at[n], sw.at[n])

    chunks = [(wq, i) for i in range(nq)] + [(wk, i) for i in range(nk)] + [(wv, i) for i in range(nv)]
    for n in range(AHEAD):
        weight(*chunks[n], n).start()

    def load(n):
        r, t = pl.ds(n * RB, RB), n % RING
        return pltpu.make_async_copy(kc.at[r], kbuf.at[t], sk.at[t]), pltpu.make_async_copy(vc.at[r], vbuf.at[t], sv.at[t])

    def store(n):
        r, t = pl.ds(n * RB, RB), n % RING
        return pltpu.make_async_copy(kbuf.at[t], ko.at[r], tk.at[t]), pltpu.make_async_copy(vbuf.at[t], vo.at[r], tv.at[t])

    def mixed(n):
        r = pl.ds(n * (RB // 2), RB // 2)
        return pltpu.make_async_copy(mix_ref.at[r], mix_out.at[r], smix.at[n])

    eye = lax.broadcasted_iota(jnp.int32, (rows, rows), 0) == lax.broadcasted_iota(jnp.int32, (rows, rows), 1)
    lens_f = lens_ref[...].astype(jnp.float32).reshape(1, rows)
    pos = jnp.sum(jnp.where(eye, lens_f, 0.0), axis=1, keepdims=True)
    angles = pos * freq_ref[...]
    half = lax.broadcasted_iota(jnp.int32, (rows, 128), 1) < 64
    cos_s[...] = jnp.cos(angles)
    sin_a = jnp.sin(angles)
    sin_s[...] = jnp.where(half, -sin_a, sin_a)
    st_ref[...] = jnp.zeros_like(st_ref)

    cx.wait()
    gain = g_ref[...].astype(jnp.float32).reshape(1, dim)

    def norm(i, carry):
        r = pl.ds(pl.multiple_of(i * 32, 32), 32)
        xf = xb[r, :].astype(jnp.float32)
        inv = lax.rsqrt(jnp.mean(xf * xf, axis=-1, keepdims=True) + NORM_EPS)
        u[r, :] = (xf * inv * gain).astype(jnp.bfloat16)
        return carry

    lax.fori_loop(0, rows // 32, norm, 0)

    def rope(t):
        return (t * cos_s[...] + pltpu.roll(t, 64, 1) * sin_s[...]).astype(jnp.bfloat16).astype(jnp.float32)

    early = [lambda n=n: weight(*chunks[n], n).start() for n in range(AHEAD, len(chunks))]
    early += [lambda n=n: [cp.start() for cp in load(n)] for n in range(min(RING, blocks))]
    per = WN // 128
    for n, (w, i) in enumerate(chunks):
        weight(w, i, n).wait()
        early.pop(0)()
        y = jnp.dot(u[...], wbuf[n], preferred_element_type=jnp.float32).astype(jnp.bfloat16).astype(jnp.float32)
        for t in range(per):
            head = y[:, t * 128 : (t + 1) * 128]
            head = head if w is wv else rope(head)
            if w is wq:
                q_s[pl.ds(i * per + t, rows, stride=16), :] = head
            else:
                dst = kn_s if w is wk else vn_s
                for again in (0, 4):
                    dst[pl.ds(i * per + t + again, rows, stride=8), :] = head
    for go in early:
        go()

    row_pos = base + lax.broadcasted_iota(jnp.int32, (128, 128), 0) // 4
    ri = lax.broadcasted_iota(jnp.int32, (32, 256), 0)
    ci = lax.broadcasted_iota(jnp.int32, (32, 256), 1)
    same = jnp.logical_and(ri // 16 == ci // 128, (ri % 16) // 4 == ci % 4)
    col_pos = jnp.where(same, base + (ci % 128) // 4, 1 << 30)
    upper = ri < 16
    lane = lax.broadcasted_iota(jnp.int32, (32, 128), 1)
    scale = 128.0 ** -0.5

    for n in range(blocks):
        slot = n % RING
        for cp in load(n):
            cp.wait()

        def group(g, carry, n=n, slot=slot):
            m_all, l_all = st_ref[0], st_ref[1]
            for j in range(PAIRS):
                local = g * PAIRS + j
                pair = n * (RB // 2) + local
                p0 = lens_s[2 * pair]
                p1 = lens_s[2 * pair + 1]
                ks, vs = [], []
                for t, p in ((0, p0), (1, p1)):
                    b = 2 * local + t
                    new = pl.ds(pl.multiple_of(8 * (2 * pair + t), 8), 8)
                    hit = row_pos == p
                    for buf, fresh, acc in ((kbuf, kn_s, ks), (vbuf, vn_s, vs)):
                        old = buf[slot, b].astype(jnp.float32)
                        add = jnp.broadcast_to(fresh[new, :][None], (16, 8, 128)).reshape(128, 128)
                        val = jnp.where(hit, add, old).astype(jnp.bfloat16)
                        buf[slot, b] = val
                        acc.append(val)
                kk = jnp.concatenate(ks, axis=0)
                vv = jnp.concatenate(vs, axis=0)
                q = q_s[pl.ds(pl.multiple_of(32 * pair, 32), 32), :].astype(jnp.bfloat16)
                s = lax.dot_general(q, kk, (((1,), (1,)), ((), ())), preferred_element_type=jnp.float32) * scale
                valid = col_pos <= jnp.where(upper, p0, p1)
                s = jnp.where(valid, s, -1e30)
                m = jnp.max(s, axis=1, keepdims=True)
                w = jnp.where(valid, jnp.exp(s - m), 0.0)
                l = jnp.sum(w, axis=1, keepdims=True)
                mix_ref[pair, :16] = jnp.dot(w[:16, :128].astype(jnp.bfloat16), vs[0], preferred_element_type=jnp.float32)
                mix_ref[pair, 16:] = jnp.dot(w[16:, 128:].astype(jnp.bfloat16), vs[1], preferred_element_type=jnp.float32)
                m_all = jnp.where(lane == pair, m, m_all)
                l_all = jnp.where(lane == pair, l, l_all)
            st_ref[0] = m_all
            st_ref[1] = l_all
            return carry

        lax.fori_loop(0, RB // 2 // PAIRS, group, 0)
        for cp in store(n):
            cp.start()
        mixed(n).start()
        if n >= 1 and n - 1 + RING < blocks:
            for cp in store(n - 1):
                cp.wait()
            for cp in load(n - 1 + RING):
                cp.start()
    for n in range(blocks - RING, blocks):
        for cp in store(n):
            cp.wait()
    for n in range(blocks):
        mixed(n).wait()


def attend_call(seq_lens, freq, g_attn, x_tok, wq, wk, wv, k2, v2):
    rows, dim = x_tok.shape
    chunks = (wq.shape[1] + wk.shape[1] + wv.shape[1]) // WN
    batch = k2.shape[0]
    vm = pl.BlockSpec(memory_space=pltpu.VMEM)
    hbm = pl.BlockSpec(memory_space=pl.ANY)
    f32, bf16 = jnp.float32, jnp.bfloat16
    dma = pltpu.SemaphoreType.DMA
    return pl.pallas_call(
        attend_kernel,
        in_specs=[pl.BlockSpec(memory_space=pltpu.SMEM), vm, vm, vm] + [hbm] * 6,
        out_specs=[hbm, hbm, hbm, vm],
        out_shape=[
            jax.ShapeDtypeStruct(k2.shape, bf16),
            jax.ShapeDtypeStruct(v2.shape, bf16),
            jax.ShapeDtypeStruct((batch // 2, 32, 128), f32),
            jax.ShapeDtypeStruct((2, 32, 128), f32),
        ],
        scratch_shapes=[
            pltpu.VMEM((batch // 2, 32, 128), f32),
            dma((batch // RB,)),
            pltpu.VMEM((rows, dim), bf16),
            pltpu.VMEM((rows, dim), bf16),
            pltpu.VMEM((chunks, dim, WN), bf16),
            pltpu.VMEM((batch * 16, 128), f32),
            pltpu.VMEM((batch * 8, 128), f32),
            pltpu.VMEM((batch * 8, 128), f32),
            pltpu.VMEM((rows, 128), f32),
            pltpu.VMEM((rows, 128), f32),
            pltpu.VMEM((RING, RB, 128, 128), bf16),
            pltpu.VMEM((RING, RB, 128, 128), bf16),
            dma, dma((chunks,)), dma((RING,)), dma((RING,)), dma((RING,)), dma((RING,)),
        ],
        compiler_params=pltpu.CompilerParams(vmem_limit_bytes=VMEM_LIMIT),
        name="attend",
    )(seq_lens, seq_lens, freq, g_attn, x_tok, wq, wk, wv, k2, v2)


def coords():
    z = lax.axis_index("tp")
    sp = lax.axis_index("sp")
    return z, sp // 4, (sp // 2) % 2, sp % 2


def device(z, y, x, c):
    return (z, y * 4 + x * 2 + c)


def flip(a, on):
    return 1 - a if on else a


def greet(peers):
    barrier = pltpu.get_barrier_semaphore()
    for p in peers:
        pl.semaphore_signal(barrier, inc=1, device_id=p, device_id_type=MESH)
    pl.semaphore_wait(barrier, len(peers))


def remote(src, dst, send, recv, dev):
    return pltpu.make_async_remote_copy(src_ref=src, dst_ref=dst, send_sem=send, recv_sem=recv, device_id=dev, device_id_type=MESH)


def combine_kernel(mix_hbm, st_own, wo, part_ref, own, so, o_s, wbuf, sw, got1, st1, comb, stc, stn, got2, st2, s1, r1, s2, r2):
    z, y, x, c = coords()
    partner = device(z, y, x, 1 - c)
    chips = [(y, x), (y, 1 - x), (1 - y, x), (1 - y, 1 - x)]
    y1, x1 = y + c * (1 - 2 * y), x + (1 - c) * (1 - 2 * x)
    y2, x2 = y + (1 - c) * (1 - 2 * y), x + c * (1 - 2 * x)
    dev1, dev2 = device(z, y1, x1, c), device(z, y2, x2, c)
    k1, k2 = 1 + c, 2 - c
    kept = {}
    for k in (3, 1, 2, 0):
        b, a = chips[k]
        kept[k] = pltpu.make_async_copy(mix_hbm.at[pl.ds(16 * (b * 4 + a * 2 + c), 16)], own.at[k], so.at[k])
    greet([partner, dev1, dev2])
    stat1 = remote(st_own, st1, s1.at[4], r1.at[4], partner)
    stat1.start()
    first = {}
    for k in (3, 1, 2, 0):
        b, a = chips[k]
        start = 16 * (b * 4 + a * 2 + 1 - c)
        first[k] = remote(mix_hbm.at[pl.ds(start, 16)], got1.at[k], s1.at[k], r1.at[k], partner)
        first[k].start()
        kept[k].start()
    weights = [pltpu.make_async_copy(wo.at[pl.ds(n * WN, WN)], wbuf.at[pl.ds(n * WN, WN)], sw.at[n]) for n in range(wo.shape[0] // WN)]

    def merge(pa, pb):
        m = jnp.maximum(pa[0], pb[0])
        fa, fb = jnp.exp(pa[0] - m), jnp.exp(pb[0] - m)
        return m, pa[1] * fa + pb[1] * fb, fa, fb

    def turned(f, b, a):
        return pltpu.roll(f, (128 - 16 * (b * 4 + a * 2 + c)) % 128, 1)

    stat1.wait_recv()
    m, l, fa, fb = merge((st_own[0], st_own[1]), (st1[0], st1[1]))
    stc[0] = m
    stc[1] = l
    stat2 = remote(stc, st2.at[0], s2.at[3], r2.at[3], dev1)
    stat2.start()

    def pair_sum(k):
        b, a = chips[k]
        ga, gb = turned(fa, b, a), turned(fb, b, a)
        kept[k].wait()
        first[k].wait_recv()
        for j in range(16):
            comb[k, j] = own[k, j] * ga[:, j : j + 1] + got1[k, j] * gb[:, j : j + 1]

    def hop(src, dst, dev):
        cp = remote(comb.at[src], got2.at[dst], s2.at[dst], r2.at[dst], dev)
        cp.start()
        return cp

    pair_sum(3)
    far = hop(3, 0, dev1)
    pair_sum(1)
    pair_sum(2)
    direct = hop(k1, 1, dev1)
    for cp in weights:
        cp.start()
    pair_sum(0)
    stat2.wait_recv()
    m, l, fa, fb = merge((m, l), (st2[0, 0], st2[0, 1]))
    stn[0] = m
    stn[1] = l
    stat3 = remote(stn, st2.at[1], s2.at[4], r2.at[4], dev2)
    stat3.start()
    ga, gb = turned(fa, y2, x2), turned(fb, y2, x2)
    far.wait_recv()
    for j in range(16):
        comb[4, j] = comb[k2, j] * ga[:, j : j + 1] + got2[0, j] * gb[:, j : j + 1]
    second = hop(4, 2, dev2)
    stat3.wait_recv()
    _, l, na, nb = merge((m, l), (st2[1, 0], st2[1, 1]))
    fa, fb, nb, l = turned(fa * na, y, x), turned(fb * na, y, x), turned(nb, y, x), turned(l, y, x)
    direct.wait_recv()
    second.wait_recv()
    for j in range(16):
        at = slice(j, j + 1)
        acc = comb[0, j] * fa[:, at] + got2[1, j] * fb[:, at] + got2[2, j] * nb[:, at]
        o_s[32 * j : 32 * j + 32, :] = acc / l[:, at]
    o = jnp.concatenate([o_s[pl.ds(h, 32, stride=16), :].astype(jnp.bfloat16) for h in range(16)], axis=1)
    for cp in weights:
        cp.wait()
    for n in range(wo.shape[1] // WN):
        cols = slice(n * WN, (n + 1) * WN)
        part_ref[:, cols] = jnp.dot(o, wbuf[:, cols], preferred_element_type=jnp.float32)
    for cp in list(first.values()) + [stat1, stat2, stat3, far, direct, second]:
        cp.wait_send()


def combine_call(mix, stat, wo):
    vm = pl.BlockSpec(memory_space=pltpu.VMEM)
    f32 = jnp.float32
    depth, dim = wo.shape
    return pl.pallas_call(
        combine_kernel,
        out_shape=jax.ShapeDtypeStruct((32, dim), f32),
        in_specs=[pl.BlockSpec(memory_space=pl.ANY), vm, pl.BlockSpec(memory_space=pl.ANY)],
        out_specs=vm,
        scratch_shapes=[
            pltpu.VMEM((4, 16, 32, 128), f32),
            pltpu.SemaphoreType.DMA((4,)),
            pltpu.VMEM((512, 128), f32),
            pltpu.VMEM((depth, dim), jnp.bfloat16),
            pltpu.SemaphoreType.DMA((depth // WN,)),
            pltpu.VMEM((4, 16, 32, 128), f32),
            pltpu.VMEM((2, 32, 128), f32),
            pltpu.VMEM((5, 16, 32, 128), f32),
            pltpu.VMEM((2, 32, 128), f32),
            pltpu.VMEM((2, 32, 128), f32),
            pltpu.VMEM((3, 16, 32, 128), f32),
            pltpu.VMEM((2, 2, 32, 128), f32),
            pltpu.SemaphoreType.DMA((5,)),
            pltpu.SemaphoreType.DMA((5,)),
            pltpu.SemaphoreType.DMA((5,)),
            pltpu.SemaphoreType.DMA((5,)),
        ],
        compiler_params=pltpu.CompilerParams(collective_id=0, has_side_effects=True, vmem_limit_bytes=VMEM_LIMIT),
        name="combine",
    )(mix, stat, wo)


GN = 256
PIECES = 5
KN = 1024
HELD = 4096


def hidden_kernel(part_hbm, x_hbm, g_ref, wg, wu, wd, down_hbm, hid_ref, part_s, down_s, sp, sdo, x_ref, zb, hbuf, h_s, act, gbuf, ubuf, dbuf,
                  sg, su, sdw, sx, sz, rz, ss, rs, sd, rd):
    z, y, x, c = coords()
    depth = act.shape[1]
    mine_from = (2 * x + c) * depth
    gates, downs = depth // GN, wd.shape[1] // WN

    def gate_load(w, buf, sem, n):
        r = pl.ds(n * KN, KN)
        return pltpu.make_async_copy(w.at[r, pl.ds(pl.multiple_of(mine_from, GN), depth)], buf.at[r], sem.at[n])

    def down_load(n):
        src = wd.at[pl.ds(pl.multiple_of(mine_from + n * GN, GN), GN), pl.ds(0, dbuf.shape[1])]
        return pltpu.make_async_copy(src, dbuf.at[pl.ds(n * GN, GN)], sdw.at[n])

    at = pl.multiple_of(32 * (y * 4 + x * 2 + c) + 16 * z, 16)
    cx = pltpu.make_async_copy(x_hbm.at[pl.ds(at, 16)], x_ref, sx)
    cx.start()
    cp_own = pltpu.make_async_copy(part_hbm.at[pl.ds(pl.multiple_of(16 * z, 16), 16)], part_s, sp)
    cp_own.start()
    loads = [gate_load(w, buf, sem, n) for n in range(wg.shape[0] // KN) for w, buf, sem in ((wg, gbuf, sg), (wu, ubuf, su))]
    loads += [down_load(n) for n in range(gates)]
    partner = device(z, y, x, 1 - c)
    zdev = device(1 - z, y, x, c)
    xdev = device(z, y, 1 - x, c)
    dim = zb.shape[1]
    step = dim // PIECES
    cols = [pl.ds(p * step, step) for p in range(PIECES)]
    greet([partner, zdev, xdev])
    sums = [remote(part_hbm.at[pl.ds(16 * (1 - z), 16), cols[p]], zb.at[:, cols[p]], sz.at[p], rz.at[p], zdev) for p in range(PIECES)]
    for cp in sums:
        cp.start()
    for cp in loads:
        cp.start()
    cx.wait()
    cp_own.wait()
    slot = lambda zz, xx, cc: (xx * 2 + cc) * 2 + zz
    mine = slot(z, x, c)

    def send(sl, p, dev, s, r, n):
        cp = remote(hbuf.at[sl, :, cols[p]], hbuf.at[sl, :, cols[p]], s.at[n * PIECES + p], r.at[n * PIECES + p], dev)
        cp.start()
        return cp

    over_z, over_x, over_c = {}, {}, {}
    for p in range(PIECES):
        sums[p].wait_recv()
        own = part_s[:, cols[p]] + zb[:, cols[p]]
        hid = (x_ref[:, cols[p]].astype(jnp.float32) + own).astype(jnp.bfloat16).astype(jnp.float32)
        hid_ref[:, cols[p]] = hid
        hbuf[mine, :, cols[p]] = hid
        over_z[p] = send(mine, p, zdev, ss, rs, 0)
        over_x[0, p] = send(mine, p, xdev, ss, rs, 1)
        over_c[0, p] = send(mine, p, partner, sd, rd, 0)
    sz1, sx1, sd1 = slot(1 - z, x, c), slot(z, 1 - x, c), slot(1 - z, 1 - x, c)
    for p in range(PIECES):
        over_z[p].wait_recv()
        over_x[1, p] = send(sz1, p, xdev, ss, rs, 2)
        over_c[1, p] = send(sz1, p, partner, sd, rd, 1)
    gain = g_ref[...].astype(jnp.float32).reshape(1, dim)

    def norm(k):
        hid = hbuf[k]
        inv = lax.rsqrt(jnp.mean(hid * hid, axis=-1, keepdims=True) + NORM_EPS)
        h_s[pl.ds(pl.multiple_of(16 * k, 16), 16), :] = (hid * inv * gain).astype(jnp.bfloat16)

    norm(mine)
    norm(sz1)
    for p in range(PIECES):
        over_x[0, p].wait_recv()
        over_c[2, p] = send(sx1, p, partner, sd, rd, 2)
    for p in range(PIECES):
        over_x[1, p].wait_recv()
        over_c[3, p] = send(sd1, p, partner, sd, rd, 3)
    norm(sx1)
    norm(sd1)
    for n, (zz, xx) in enumerate(((z, x), (1 - z, x), (z, 1 - x), (1 - z, 1 - x))):
        for p in range(PIECES):
            over_c[n, p].wait_recv()
        norm(slot(zz, xx, 1 - c))
    for cp in sums + list(over_z.values()) + list(over_x.values()) + list(over_c.values()):
        cp.wait_send()
    up16 = lambda t: t.astype(jnp.bfloat16).astype(jnp.float32)
    for cp in loads[: len(loads) - gates]:
        cp.wait()
    for n in range(gates):
        part = slice(n * GN, (n + 1) * GN)
        gate = up16(jnp.dot(h_s[...], gbuf[:, part], preferred_element_type=jnp.float32))
        up = up16(jnp.dot(h_s[...], ubuf[:, part], preferred_element_type=jnp.float32))
        act[:, part] = (jax.nn.silu(gate) * up).astype(jnp.bfloat16)
    def out(n):
        r = pl.ds(n * WN, WN)
        return pltpu.make_async_copy(down_s.at[:, r], down_hbm.at[:, r], sdo.at[n])

    held = dbuf.shape[1]
    rest = wd.shape[1] - held
    spare = gbuf.at[pl.ds(0, depth), pl.ds(0, rest)]
    last = pltpu.make_async_copy(wd.at[pl.ds(pl.multiple_of(mine_from, GN), depth), pl.ds(held, rest)], spare, sdw.at[gates])
    last.start()
    for cp in loads[len(loads) - gates :]:
        cp.wait()
    for n in range(downs):
        if n * WN == held:
            last.wait()
        wide = dbuf[:, n * WN : (n + 1) * WN] if n * WN < held else gbuf[:depth, n * WN - held : (n + 1) * WN - held]
        down_s[:, n * WN : (n + 1) * WN] = jnp.dot(act[...], wide, preferred_element_type=jnp.float32)
        out(n).start()
    for n in range(downs):
        out(n).wait()


def hidden_call(part, x_tok, g, wg, wu, wd, ways):
    vm = pl.BlockSpec(memory_space=pltpu.VMEM)
    f32 = jnp.float32
    dim = part.shape[1]
    dma = pltpu.SemaphoreType.DMA
    hbm = pl.BlockSpec(memory_space=pl.ANY)
    depth = wg.shape[1] // ways
    bf16 = jnp.bfloat16
    return pl.pallas_call(
        hidden_kernel,
        out_shape=[jax.ShapeDtypeStruct((128, dim), f32), jax.ShapeDtypeStruct((16, dim), f32)],
        in_specs=[hbm, hbm, vm, hbm, hbm, hbm],
        out_specs=[hbm, vm],
        scratch_shapes=[
            pltpu.VMEM((16, dim), f32),
            pltpu.VMEM((128, dim), f32),
            dma,
            dma((dim // WN,)),
            pltpu.VMEM((16, dim), bf16),
            pltpu.VMEM((16, dim), f32),
            pltpu.VMEM((8, 16, dim), f32),
            pltpu.VMEM((128, dim), bf16),
            pltpu.VMEM((128, depth), bf16),
            pltpu.VMEM((dim, depth), bf16),
            pltpu.VMEM((dim, depth), bf16),
            pltpu.VMEM((depth, HELD), bf16),
            dma((dim // KN,)), dma((dim // KN,)), dma((depth // GN + 1,)),
            dma, dma((PIECES,)), dma((PIECES,)), dma((3 * PIECES,)), dma((3 * PIECES,)), dma((4 * PIECES,)), dma((4 * PIECES,)),
        ],
        compiler_params=pltpu.CompilerParams(collective_id=1, has_side_effects=True, vmem_limit_bytes=VMEM_MOST),
        name="hidden",
    )(part, x_tok, g, wg, wu, wd)


COLORS = ((0, 1664), (1664, 1664), (3328, 1792))


def output_kernel(part_ref, hid_ref, y_ref, got1, acc, got2, ybuf, s1, r1, s2, r2, sl, rl, sd, rd):
    z, y, x, c = coords()
    partner = device(z, y, x, 1 - c)
    chips = [(z, x), (z, 1 - x), (1 - z, x), (1 - z, 1 - x)]
    near = [device(z, y, 1 - x, c), device(z, 1 - y, x, c), device(1 - z, y, x, c)]
    greet([partner] + near)
    slot = lambda zz, xx, cc: (xx * 2 + cc) * 2 + zz
    rows16 = lambda s: pl.ds(pl.multiple_of(16 * s, 16), 16)
    cols = [pl.ds(*color) for color in COLORS]
    z1, x1 = z + c * (1 - 2 * z), x + (1 - c) * (1 - 2 * x)
    z2, x2 = z + (1 - c) * (1 - 2 * z), x + c * (1 - 2 * x)
    dev1, dev2 = device(z1, y, x1, c), device(z2, y, x2, c)
    k1, k2 = 1 + c, 2 - c
    links, locals_, sums = {}, {}, []
    first = {}
    for p in range(3):
        for k in (3, 1, 2, 0):
            zz, xx = chips[k]
            n = 4 * p + k
            first[k, p] = remote(part_ref.at[rows16(slot(zz, xx, 1 - c)), cols[p]], got1.at[k, :, cols[p]], s1.at[n], r1.at[n], partner)
            first[k, p].start()

    def hop(src, dst, p, dev):
        n = 3 * p + dst
        cp = remote(acc.at[src, :, cols[p]], got2.at[dst, :, cols[p]], s2.at[n], r2.at[n], dev)
        cp.start()
        sums.append(cp)
        return cp

    far, direct, second = {}, {}, {}
    for p in range(3):
        for k in (3, 1, 2, 0):
            zz, xx = chips[k]
            first[k, p].wait_recv()
            acc[k, :, cols[p]] = part_ref[rows16(slot(zz, xx, c)), cols[p]] + got1[k, :, cols[p]]
        far[p] = hop(3, 0, p, dev1)
        direct[p] = hop(k1, 1, p, dev1)
    for p in range(3):
        far[p].wait_recv()
        acc[4, :, cols[p]] = acc[k2, :, cols[p]] + got2[0, :, cols[p]]
        second[p] = hop(4, 2, p, dev2)
    mine = y * 8 + slot(z, x, c)

    def shard(mask):
        zz, yy, xx = flip(z, mask & 4), flip(y, mask & 2), flip(x, mask & 1)
        return yy * 8 + slot(zz, xx, c)

    def piece(mask, k):
        return ybuf.at[shard(mask), :, pl.ds(*COLORS[k])]

    def push(mask, k, dim):
        n = 7 * k + (mask | (1 << dim)) - 1
        cp = remote(piece(mask, k), piece(mask, k), sl.at[n], rl.at[n], near[dim])
        cp.start()
        links[k, mask | (1 << dim)] = cp

    def across(mask, k):
        n = 8 * k + mask
        cp = remote(piece(mask, k), piece(mask, k), sd.at[n], rd.at[n], partner)
        cp.start()
        locals_[k, mask] = cp

    turn = lambda k: [(k + i) % 3 for i in range(3)]
    for k in range(3):
        direct[k].wait_recv()
        near_sum = acc[0, :, cols[k]] + got2[1, :, cols[k]]
        second[k].wait_recv()
        total = near_sum + got2[2, :, cols[k]]
        ybuf[mine, :, cols[k]] = (hid_ref[:, cols[k]] + total).astype(jnp.bfloat16).astype(jnp.float32)
        for i in range(3):
            push(0, k, turn(k)[i])
        across(0, k)
    for level in ((0,), (1,), (0, 1), (2,), (0, 2), (1, 2), (0, 1, 2)):
        for k in range(3):
            dims = turn(k)
            mask = sum(1 << dims[i] for i in level)
            links[k, mask].wait_recv()
            for i in range(max(level) + 1, 3):
                push(mask, k, dims[i])
            across(mask, k)
    for cp in locals_.values():
        cp.wait_recv()
    for s in range(16):
        y_ref[pl.ds(16 * s, 16), :] = ybuf[s].astype(jnp.bfloat16)
    for cp in list(first.values()) + sums + list(links.values()) + list(locals_.values()):
        cp.wait_send()


def output_call(part, hid):
    vm = pl.BlockSpec(memory_space=pltpu.VMEM)
    f32 = jnp.float32
    dim = part.shape[1]
    dma = pltpu.SemaphoreType.DMA
    return pl.pallas_call(
        output_kernel,
        out_shape=jax.ShapeDtypeStruct((256, dim), jnp.bfloat16),
        in_specs=[vm, vm],
        out_specs=vm,
        scratch_shapes=[
            pltpu.VMEM((4, 16, dim), f32),
            pltpu.VMEM((5, 16, dim), f32),
            pltpu.VMEM((3, 16, dim), f32),
            pltpu.VMEM((16, 16, dim), f32),
            dma((12,)), dma((12,)), dma((9,)), dma((9,)), dma((21,)), dma((21,)), dma((24,)), dma((24,)),
        ],
        compiler_params=pltpu.CompilerParams(collective_id=2, has_side_effects=True, vmem_limit_bytes=28 * 1024 * 1024),
        name="output",
    )(part, hid)


def solution(mesh):
    cache_spec = P(None, "sp", "tp", None)
    col_spec = P(None, "tp")
    row_spec = P("tp", None)
    full_spec = P()

    def local_step(x_tok, seq_lens, k_blk, v_blk, g_attn, wq_loc, wk_loc, wv_loc, wo_loc, g_mlp, wg_loc, wu_loc, wd_loc):
        batch, seq_blk, kv_loc, head_dim = k_blk.shape
        q_loc = wq_loc.shape[1] // head_dim
        freq = ROPE_BASE ** (np.arange(head_dim // 2, dtype=np.float64) * (-2.0 / head_dim))
        freq = jnp.asarray(np.concatenate([freq, freq])[None].astype(np.float32))
        flat = (batch, seq_blk * kv_loc, head_dim)
        k_out, v_out, mix, stat = attend_call(seq_lens, freq, g_attn, x_tok, wq_loc, wk_loc, wv_loc, k_blk.reshape(flat), v_blk.reshape(flat))
        part = combine_call(mix, stat, wo_loc)
        down, hid = hidden_call(part, x_tok, g_mlp, wg_loc, wu_loc, wd_loc, 4)
        y_out = output_call(down, hid)
        return y_out, k_out.reshape(k_blk.shape), v_out.reshape(v_blk.shape)

    return jax.shard_map(local_step, mesh=mesh, in_specs=(full_spec, full_spec, cache_spec, cache_spec, full_spec, col_spec, col_spec, col_spec, row_spec, full_spec, col_spec, col_spec, row_spec), out_specs=(full_spec, cache_spec, cache_spec), check_vma=False)
```
